32 devices in a mesh: sp: 4 (over y, x), fsdp: 8 (over z, core).
Axes of the slice: x: 2, y: 2, z: 4, core: 2. Of those that a mesh axis runs over, the one named last changes fastest.
Arguments:
- tokens: bfloat16 [2, 8, 1536, 1024], P(None, 'fsdp', 'sp'), may hold values from -6 to 6
- cotangent: bfloat16 [2, 8, 1536, 1024], P(None, 'fsdp', 'sp'), may hold values from -6 to 6
- destination: int32 [2, 8, 1536], P(None, 'fsdp', 'sp'), may hold values from 0 to 3071, as said below
- seq_lengths: int32 [2, 8, 3], P(None, 'fsdp'), may hold values from 1 to 1024, 1536 in all within a row
- qkv_weight: bfloat16 [1024, 3072], P('fsdp'), may hold values from -0.1875 to 0.1875
- output_weight: bfloat16 [1024, 1024], P('fsdp'), may hold values from -3 to 3
- input_weight: bfloat16 [1024, 5248], P('fsdp'), may hold values from -0.1875 to 0.1875
- mlp_weight: bfloat16 [2624, 1024], P(None, 'fsdp'), may hold values from -0.125 to 0.125
- first_gain: bfloat16 [1024], P('fsdp'), may hold values from 0.25 to 1.75
- second_gain: bfloat16 [1024], P('fsdp'), may hold values from 0.25 to 1.75
Outputs:
- layer_output: bfloat16 [2, 8, 1536, 1024], P(None, 'fsdp', 'sp')
- input_grad: bfloat16 [2, 8, 1536, 1024], P(None, 'fsdp', 'sp')
- qkv_weight_grad: float32 [1024, 3072], P('fsdp')
- output_weight_grad: float32 [1024, 1024], P('fsdp')
- input_weight_grad: float32 [1024, 5248], P('fsdp')
- mlp_weight_grad: float32 [2624, 1024], P(None, 'fsdp')
- first_gain_grad: float32 [1024], P('fsdp')
- second_gain_grad: float32 [1024], P('fsdp')
The draws below stay inside these ranges and needn't reach their ends.
Inputs may be any that keep to these rules, and one draw needn't show every extreme that they name: destination[b, f, p] = g * 384 + r sends the row to place (p // 384) * 384 + r of group g; for each b and each block of 384 places with the same p // 384, over all f these places are each reached exactly once, and the rows of one f in that block send exactly 48 rows to each group. `seq_lengths`: the lengths of one group sum to 1536.
All inputs are finite; a program needn't handle non-finite values.
Results may differ from the reference program's by a relative error of at most 0.017.
Values may be sent and summed in bfloat16 or wider, within the bound.
A program may use at most 384 MiB of HBM per device.

```python
import math
from functools import partial
import jax
import jax.numpy as jnp
import numpy as np
from jax import lax

D = 1024
HEADS = 16
HEAD_DIM = 64
FF = 2624
TOK_DEV = 384
N_MB = 2
NSEQ = 3
GROUP = 1536
GROUPS = 8
LONGEST = 1024


def slab_destination(slab_key):
    per_peer = TOK_DEV // GROUPS
    slots = jnp.arange(TOK_DEV, dtype=jnp.int32)
    owners = slots // per_peer
    offsets = slots % per_peer
    key_order, key_place = jax.random.split(slab_key)
    orders = jax.vmap(lambda inner_key: jax.random.permutation(inner_key, GROUPS))(jax.random.split(key_order, GROUPS)).astype(jnp.int32)
    targets = owners[None, :] * TOK_DEV + jnp.transpose(orders[owners, :]) * per_peer + offsets[None, :]
    places = jax.vmap(lambda inner_key: jax.random.permutation(inner_key, TOK_DEV))(jax.random.split(key_place, GROUPS)).astype(jnp.int32)
    sources = jnp.arange(GROUPS, dtype=jnp.int32)[:, None]
    return jnp.zeros((GROUPS, TOK_DEV), jnp.int32).at[sources, places].set(targets)


def draw_destination(key, part):
    slab_count = GROUP // TOK_DEV
    slab_keys = jax.random.split(key, N_MB * slab_count)
    drawn = jax.vmap(slab_destination)(slab_keys)
    drawn = drawn.reshape(N_MB, slab_count, GROUPS, TOK_DEV)
    return jnp.transpose(drawn, (0, 2, 1, 3)).reshape(N_MB, GROUPS, GROUP).astype(jnp.int32)


def block_scale(rng, shape, shards, low, top_value):
    level, own = 1.0, jax.random.fold_in(rng, 6)
    for axis_at, blocks in shards:
        draws = jnp.exp(jax.random.uniform(jax.random.fold_in(own, axis_at), (blocks,), jnp.float32, low / len(shards), top_value / len(shards)))
        level = level * jnp.repeat(draws, shape[axis_at] // blocks).reshape([-1 if axis == axis_at else 1 for axis in range(len(shape))])
    return level


def split_up(number_of, total, limit, lean):
    loads = [(1 << 20) // math.isqrt(rank ** lean) + 1 for rank in range(2, number_of + 1)]
    rest, given = total - limit - (number_of - 1), [1] * (number_of - 1)
    while rest > 0:
        movable = [i for i in range(number_of - 1) if given[i] < limit]
        mass, remaining = sum([loads[i] for i in movable]), rest
        for i in movable:
            extra = min(limit - given[i], max(1, remaining * loads[i] // mass), rest)
            given[i] = given[i] + extra
            rest = rest - extra
    return np.array([limit] + given)


def ragged_sizes(own_key, amount, total, most, skew):
    if amount == 2:
        one = jax.random.randint(own_key, (), max(1, total - most), min(most, total - 1) + 1)
        return jnp.stack([one, total - one])
    sizes = jnp.asarray(split_up(amount, total, most, skew), jnp.int32)
    pairs = (amount - 1) // 2
    source_of, sink = sizes[1:1 + 2 * pairs:2], sizes[2:2 + 2 * pairs:2]
    margin = jnp.minimum(source_of - 1, most - sink)
    moved = jax.random.randint(jax.random.fold_in(own_key, 1), (pairs,), 0, 1 << 20) % (margin + 1)
    sizes = sizes.at[1:1 + 2 * pairs:2].set(source_of - moved).at[2:2 + 2 * pairs:2].set(sink + moved)
    return sizes[jax.random.permutation(jax.random.fold_in(own_key, 2), amount)]


def centred(key, shape, deviation, reach, pieces=(), held_as=jnp.bfloat16):
    factor_of = block_scale(key, shape, pieces, -0.22, 0.18) if pieces else 1.0
    values = jax.random.normal(key, shape, jnp.float32) * deviation * factor_of
    return jnp.minimum(jnp.maximum(values, -reach), reach).astype(held_as)


def setup_inputs(seed: int = 0) -> dict:
    key_of = jax.random.split(jax.random.key(seed), 11)
    tokens = centred(key_of[0], (N_MB, GROUPS, GROUP, D), 1.0, 6.0, ((1, 8), (2, 4)))
    cotangent = centred(key_of[1], (N_MB, GROUPS, GROUP, D), 1.0, 6.0, ((1, 8), (2, 4)))
    destination = draw_destination(jax.random.fold_in(key_of[10], 71), 0)
    seq_lengths = jax.vmap(lambda own: ragged_sizes(own, NSEQ, GROUP, LONGEST, 1))(jax.random.split(key_of[3], N_MB * GROUPS)).reshape((N_MB, GROUPS, NSEQ)).astype(jnp.int32)
    qkv_weight = centred(key_of[4], (D, 3 * D), D ** -0.5, 0.1875, ((0, 8),))
    output_weight = centred(key_of[5], (D, D), (max(2, D // 256)) ** -0.5, 3.0, ((0, 8),))
    input_weight = centred(key_of[6], (D, 2 * FF), D ** -0.5, 0.1875, ((0, 8),))
    mlp_weight = centred(key_of[7], (FF, D), FF ** -0.5, 0.125, ((1, 8),))
    first_gain = jnp.clip(1.0 + 0.15 * jax.random.normal(key_of[8], (D,), jnp.float32), 0.25, 1.75).astype(jnp.bfloat16)
    second_gain = jnp.clip(1.0 + 0.15 * jax.random.normal(key_of[9], (D,), jnp.float32), 0.25, 1.75).astype(jnp.bfloat16)
    return {"tokens": tokens, "cotangent": cotangent, "destination": destination, "seq_lengths": seq_lengths, "qkv_weight": qkv_weight, "output_weight": output_weight, "input_weight": input_weight, "mlp_weight": mlp_weight, "first_gain": first_gain, "second_gain": second_gain}


norm_epsilon = 1e-05
rotary_base = 160000.0
masked_score = -1e+30
highest = lax.Precision.HIGHEST

@jax.custom_vjp
def low(v):
    return lax.optimization_barrier(v.astype(jnp.bfloat16)).astype(jnp.float32)

@jax.custom_vjp
def low_back(v):
    return v

def low_keep(v):
    return (low(v), None)

def low_pass(kept, grad):
    return (grad,)

def back_keep(v):
    return (v, None)

def back_low(kept, grad):
    return (low(grad),)
low.defvjp(low_keep, low_pass)
low_back.defvjp(back_keep, back_low)

def layer_norm(values, norm_gain):
    centre = values - lax.optimization_barrier(jnp.mean(values, axis=-1, keepdims=True))
    spread = lax.optimization_barrier(jnp.mean(centre * centre, axis=-1, keepdims=True))
    return centre * lax.rsqrt(spread + norm_epsilon) * norm_gain

def rotary_tables(places, head_width):
    exponents = jnp.arange(0, head_width, 2).astype(jnp.float32) / head_width
    inverse_freq = 1.0 / rotary_base ** exponents
    angles = places.astype(jnp.float32)[:, None] * inverse_freq[None, :]
    angles = jnp.concatenate([angles, angles], axis=-1)
    return (jnp.cos(angles), jnp.sin(angles))

def rotary(values, cosine_table, sine_table):
    half_width = values.shape[-1] // 2
    table_shape = (values.shape[0],) + (1,) * (values.ndim - 2) + (values.shape[-1],)
    turned = jnp.concatenate([-values[..., half_width:], values[..., :half_width]], axis=-1)
    return values * cosine_table.reshape(table_shape) + turned * sine_table.reshape(table_shape)

def sequence_layout(lengths_row, positions):
    seq_ends = jnp.cumsum(lengths_row)
    passed = (positions[:, None] >= seq_ends[None, :]).astype(jnp.int32)
    seq_ids = lax.optimization_barrier(jnp.sum(passed, axis=1))
    seq_starts = lax.optimization_barrier(jnp.sum(passed * lengths_row[None, :], axis=1))
    return (seq_ids, positions - seq_starts)

def group_forward(params, inputs):
    qkv_full, out_full, in_full, mlp_full, gain_one, gain_two = params
    values, lengths_row = inputs
    group_rows = values.shape[0]
    positions = jnp.arange(group_rows, dtype=jnp.int32)
    seq_ids, places = sequence_layout(lengths_row, positions)
    cosine_table, sine_table = rotary_tables(places, HEAD_DIM)
    normed_one = low(layer_norm(values, gain_one))
    projected = low_back(jnp.dot(normed_one, qkv_full, precision=highest)).reshape(group_rows, 3, HEADS, HEAD_DIM)
    query_heads = low(low_back(rotary(projected[:, 0], cosine_table, sine_table)))
    key_heads = low(low_back(rotary(projected[:, 1], cosine_table, sine_table)))
    value_heads = low(low_back(projected[:, 2]))
    row_block = min(512, group_rows)
    score_scale = HEAD_DIM ** (-0.5)

    def attend(block_inputs):
        block_queries, block_ids = block_inputs
        raw_scores = jnp.einsum('qhd,khd->hqk', block_queries, key_heads, precision=highest) * score_scale
        scores = low_back(raw_scores)
        same_seq = block_ids[:, None] == seq_ids[None, :]
        masked = jnp.where(same_seq[None], scores, masked_score)
        row_max = lax.optimization_barrier(jnp.max(masked, axis=-1, keepdims=True))
        exponent_terms = jnp.exp(masked - row_max)
        softmax_weights = low(exponent_terms / lax.optimization_barrier(jnp.sum(exponent_terms, axis=-1, keepdims=True)))
        return jnp.einsum('hqk,khd->qhd', softmax_weights, value_heads, precision=highest)
    blocked = (query_heads.reshape(group_rows // row_block, row_block, HEADS, HEAD_DIM), seq_ids.reshape(group_rows // row_block, row_block))
    mixed = lax.map(jax.checkpoint(attend), blocked).reshape(group_rows, HEADS * HEAD_DIM)
    attended = low(low_back(mixed))
    middle = values + low_back(jnp.dot(attended, out_full, precision=highest))
    normed_two = low(layer_norm(middle, gain_two))
    lifted = jnp.dot(normed_two, in_full, precision=highest)
    gate_part = low_back(lifted[:, :FF])
    up_part = low_back(lifted[:, FF:])
    hidden = low(jax.nn.gelu(gate_part, approximate=False) * up_part)
    return middle + low_back(jnp.dot(hidden, mlp_full, precision=highest))

def reference(tokens, cotangent, destination, seq_lengths, qkv_weight, output_weight, input_weight, mlp_weight, first_gain, second_gain):
    batch_ids = jnp.arange(N_MB, dtype=jnp.int32)[:, None, None]
    group_ids = destination // TOK_DEV
    place_ids = jnp.arange(GROUP, dtype=jnp.int32)[None, None, :] // TOK_DEV * TOK_DEV + destination % TOK_DEV
    empty = jnp.zeros((N_MB, GROUPS, GROUP, D), jnp.float32)
    owned = empty.at[batch_ids, group_ids, place_ids].set(tokens.astype(jnp.float32))
    owned_cot = empty.at[batch_ids, group_ids, place_ids].set(cotangent.astype(jnp.float32))
    params = (qkv_weight.astype(jnp.float32), output_weight.astype(jnp.float32), input_weight.astype(jnp.float32), mlp_weight.astype(jnp.float32), first_gain.astype(jnp.float32), second_gain.astype(jnp.float32))

    def forward(weight_set, owned_tokens):
        flat_tokens = owned_tokens.reshape(N_MB * GROUPS, GROUP, D)
        flat_lengths = seq_lengths.reshape(N_MB * GROUPS, NSEQ)
        outputs = lax.map(jax.checkpoint(partial(group_forward, weight_set)), (flat_tokens, flat_lengths))
        return outputs.reshape(N_MB, GROUPS, GROUP, D)
    owned_out, pullback = jax.vjp(forward, params, owned)
    param_grads, token_grads = pullback(owned_cot)
    layer_output = owned_out[batch_ids, group_ids, place_ids].astype(jnp.bfloat16)
    input_grad = token_grads[batch_ids, group_ids, place_ids].astype(jnp.bfloat16)
    return (layer_output, input_grad, param_grads[0], param_grads[1], param_grads[2], param_grads[3], param_grads[4], param_grads[5])
```

```python
import jax
import jax.numpy as jnp
from jax import lax
from jax.sharding import Mesh, PartitionSpec as P

HEADS = 16
HEAD_DIM = 64
norm_epsilon = 1e-05
rotary_base = 160000.0
masked_score = -1e30
BF = jnp.bfloat16
F32 = jnp.float32
SWAP = [(0, 1), (1, 0)]


def mm(a, b, dims=((1,), (0,))):
    return lax.dot_general(a, b, (dims, ((), ())), preferred_element_type=F32)


def swap(x):
    return lax.ppermute(x, "core", SWAP)


def norm_parts(values):
    centre = values - jnp.mean(values, axis=-1, keepdims=True)
    spread = jnp.mean(centre * centre, axis=-1, keepdims=True)
    scale = lax.rsqrt(spread + norm_epsilon)
    return centre * scale, scale


def norm_back(grad, gain, n, scale):
    h = grad * gain
    back = scale * (
        h - jnp.mean(h, axis=-1, keepdims=True) - n * jnp.mean(h * n, axis=-1, keepdims=True)
    )
    return back, jnp.sum(grad * n, axis=0)


def rotary_tables(places):
    exponents = jnp.arange(0, HEAD_DIM, 2).astype(F32) / HEAD_DIM
    inverse_freq = 1.0 / rotary_base**exponents
    angles = places.astype(F32)[:, None] * inverse_freq[None, :]
    angles = jnp.concatenate([angles, angles], axis=-1)
    return jnp.cos(angles), jnp.sin(angles)


def turn(u):
    half = HEAD_DIM // 2
    return jnp.concatenate([-u[..., half:], u[..., :half]], axis=-1)


def turn_back(u):
    half = HEAD_DIM // 2
    return jnp.concatenate([u[..., half:], -u[..., :half]], axis=-1)


def sequence_layout(lengths_row, positions):
    seq_ends = jnp.cumsum(lengths_row)
    passed = (positions[:, None] >= seq_ends[None, :]).astype(jnp.int32)
    seq_ids = jnp.sum(passed, axis=1)
    seq_starts = jnp.sum(passed * lengths_row[None, :], axis=1)
    return seq_ids, positions - seq_starts


def attend(q, k, v, seq_ids):
    rows, heads = q.shape[0], q.shape[1]
    same = seq_ids[:, None] == seq_ids[None, :]
    out, lse = [], []
    for at in range(0, rows, 512):
        raw = jnp.einsum("qhd,khd->hqk", q[at : at + 512], k, preferred_element_type=F32) * 0.125
        masked = jnp.where(same[at : at + 512][None], raw, masked_score)
        top = jnp.max(masked, axis=-1, keepdims=True)
        terms = jnp.exp(masked - top)
        total = jnp.sum(terms, axis=-1, keepdims=True)
        low = (terms / total).astype(BF)
        out.append(jnp.einsum("hqk,khd->qhd", low, v, preferred_element_type=F32))
        lse.append(top + jnp.log(total))
    return jnp.concatenate(out, 0).astype(BF).reshape(rows, -1), jnp.concatenate(lse, 1)


def attend_back(q, k, v, lse, grad_out, seq_ids):
    rows = q.shape[0]
    same = seq_ids[:, None] == seq_ids[None, :]
    gq, gk, gv = [], 0.0, 0.0
    for at in range(0, rows, 512):
        cut = slice(at, at + 512)
        raw = jnp.einsum("qhd,khd->hqk", q[cut], k, preferred_element_type=F32) * 0.125
        masked = jnp.where(same[cut][None], raw, masked_score)
        probs = jnp.exp(masked - lse[:, cut])
        gv = gv + jnp.einsum(
            "hqk,qhd->khd", probs.astype(BF), grad_out[cut], preferred_element_type=F32
        )
        gp = jnp.einsum("qhd,khd->hqk", grad_out[cut], v, preferred_element_type=F32)
        gs = (probs * (gp - jnp.sum(probs * gp, axis=-1, keepdims=True))).astype(BF)
        gq.append(jnp.einsum("hqk,khd->qhd", gs, k, preferred_element_type=F32) * 0.125)
        gk = gk + jnp.einsum("hqk,qhd->khd", gs, q[cut], preferred_element_type=F32) * 0.125
    return jnp.concatenate(gq, 0).astype(BF), gk.astype(BF), gv.astype(BF)


def on_device(
    tokens,
    cotangent,
    destination,
    seq_lengths,
    qkv_weight,
    output_weight,
    input_weight,
    mlp_weight,
    first_gain,
    second_gain,
):
    sp_count, q_count = lax.axis_size("sp"), lax.axis_size("q")
    s, c = lax.axis_index("sp"), lax.axis_index("core")
    batches, _, block, width = tokens.shape
    groups = 2 * q_count
    each = block // groups
    shard = qkv_weight.shape[0]
    part = 2 * shard // sp_count
    half_ff = mlp_weight.shape[0] // 2
    half_width = width // 2
    rows = 2 * block

    owner = s // (sp_count // 2)
    first_row = (s % (sp_count // 2)) * part

    def piece(k):
        def rows_of(w):
            return lax.dynamic_slice_in_dim(w, first_row, part, 0)

        def cols(w, parts):
            w = rows_of(w).reshape(part, parts, 2, -1)
            return lax.dynamic_index_in_dim(w, k, 2, keepdims=False).reshape(part, -1)

        return (
            cols(qkv_weight, 3),
            cols(output_weight, 1),
            cols(input_weight, 2),
            cols(mlp_weight.T, 1),
        )

    mine, theirs = piece(c), piece(1 - c)
    is_owner = c == owner
    gathered = []
    for a, b in zip(mine, theirs):
        part_w = jnp.where(is_owner, a, swap(b))
        gathered.append(lax.all_gather(part_w, ("q", "sp"), axis=0, tiled=True))
    w_qkv, w_out_half, w_in, w_mlp = gathered
    w_gate, w_up = w_in[:, :half_ff], w_in[:, half_ff:]
    w_out_other = swap(w_out_half)
    w_out = jnp.where(
        c == 0,
        jnp.concatenate([w_out_half, w_out_other], 1),
        jnp.concatenate([w_out_other, w_out_half], 1),
    )
    w_out_rows = w_out.reshape(2, half_width, width)
    w_out_own = lax.dynamic_index_in_dim(w_out_rows, c, 0, keepdims=False)
    w_out_far = lax.dynamic_index_in_dim(w_out_rows, 1 - c, 0, keepdims=False)
    gains = lax.all_gather(
        jnp.stack([first_gain, second_gain]), ("q", "core"), axis=1, tiled=True
    ).astype(F32)
    gain_one, gain_two = gains[0], gains[1]

    dest = destination[:, 0]
    group_of, slot_of = dest // block, dest % block
    idx = jnp.arange(block, dtype=jnp.int32)
    before = (group_of[:, :, None] == group_of[:, None, :]) & (idx[None, None, :] < idx[None, :, None])
    place = group_of * each + jnp.sum(before.astype(jnp.int32), axis=-1)
    picks = idx[None, :, None] == place[:, None, :]
    sort_low = picks.astype(BF)
    slots = jnp.sum(jnp.where(picks, slot_of[:, None, :], 0), axis=-1)
    all_slots = lax.all_gather(slots, ("sp", "q", "core"), axis=0)
    all_slots = all_slots.reshape(sp_count, groups, batches, groups, each)
    my_batch, my_pair = s // 2, s % 2
    my_group = 2 * lax.axis_index("q") + my_pair
    my_slots = lax.dynamic_index_in_dim(all_slots, my_batch, 2, keepdims=False)
    my_slots = lax.dynamic_index_in_dim(my_slots, my_group, 2, keepdims=False)
    my_slots = my_slots.reshape(2, 2, q_count, 2, each).transpose(0, 1, 3, 2, 4)
    my_slots = lax.dynamic_index_in_dim(my_slots, c, 0, keepdims=False).reshape(2, block)
    place_low = (idx[None, :, None] == my_slots[:, None, :]).astype(BF)

    def deal(x):
        srt = jnp.einsum("bij,bjd->bid", sort_low, x[:, 0], preferred_element_type=F32).astype(BF)
        srt = srt.reshape(batches, q_count, 2, each, width).transpose(1, 0, 2, 3, 4)
        srt = srt.reshape(q_count, sp_count, each, width)
        got = lax.all_to_all(srt, "q", 0, 0, tiled=True)
        got = lax.all_to_all(got, "sp", 1, 0, tiled=True)
        got = got.reshape(2, 2, q_count, each, width)
        own = lax.dynamic_index_in_dim(got, c, 0, keepdims=False)
        far = swap(lax.dynamic_index_in_dim(got, 1 - c, 0, keepdims=False))
        both = jnp.stack([jnp.where(c == 0, own, far), jnp.where(c == 0, far, own)], axis=1)
        both = both.reshape(2, block, width)
        return jnp.einsum("tri,tid->trd", place_low, both, preferred_element_type=F32).reshape(
            rows, width
        )

    def give_back(x):
        x = x.reshape(2, block, width)
        x = jnp.einsum("tri,trd->tid", place_low, x, preferred_element_type=F32).astype(BF)
        x = x.reshape(2, 2, q_count, each, width)
        own = lax.dynamic_index_in_dim(x, c, 1, keepdims=False)
        far = swap(lax.dynamic_index_in_dim(x, 1 - c, 1, keepdims=False))
        both = jnp.where(c == 0, jnp.stack([own, far]), jnp.stack([far, own]))
        both = both.reshape(sp_count, q_count, each, width)
        got = lax.all_to_all(both, "sp", 0, 0, tiled=True)
        got = got.reshape(sp_count, q_count, each, width).transpose(1, 0, 2, 3)
        got = lax.all_to_all(got, "q", 0, 0, tiled=True)
        got = got.reshape(q_count, batches, 2, each, width).transpose(1, 0, 2, 3, 4)
        got = got.reshape(batches, block, width)
        out = jnp.einsum("bij,bid->bjd", sort_low, got, preferred_element_type=F32)
        return out.astype(BF)[:, None]

    lengths_row = lax.dynamic_index_in_dim(seq_lengths[:, 0], my_batch, 0, keepdims=False)
    my_lengths = lax.all_gather(seq_lengths[:, 0], "core", axis=0)
    my_lengths = lax.dynamic_index_in_dim(my_lengths, my_pair, 0, keepdims=False)
    lengths_row = lax.dynamic_index_in_dim(my_lengths, my_batch, 0, keepdims=False)

    owned = deal(tokens)
    cot = deal(cotangent).astype(BF)
    positions = (c * rows + jnp.arange(2 * rows, dtype=jnp.int32)) % (2 * rows)
    seq_ids, places = sequence_layout(lengths_row, positions)
    cosine, sine = rotary_tables(places)
    cosine, sine = cosine[:, None, None], sine[:, None, None]

    norm_one, scale_one = norm_parts(owned)
    low_one = (norm_one * gain_one).astype(BF)
    low_one = jnp.concatenate([low_one, swap(low_one)], 0)
    projected = mm(low_one, w_qkv).reshape(2 * rows, 3, HEADS // 2, HEAD_DIM)
    pair = projected[:, :2]
    pair = (pair * cosine + turn(pair) * sine).astype(BF)
    q, k, v = pair[:, 0], pair[:, 1], projected[:, 2].astype(BF)
    att, lse = attend(q, k, v, seq_ids)
    att_own, att_far = att[:rows], swap(att[rows:])
    middle = owned + (mm(att_own, w_out_own) + mm(att_far, w_out_far))
    norm_two, scale_two = norm_parts(middle)
    low_two = (norm_two * gain_two).astype(BF)
    low_two = jnp.concatenate([low_two, swap(low_two)], 0)
    cot_all = jnp.concatenate([cot, swap(cot)], 0)
    gate, up = mm(low_two, w_gate), mm(low_two, w_up)
    phi = 0.5 * (1.0 + lax.erf(gate * (0.5**0.5)))
    act = gate * phi
    hidden = (act * up).astype(BF)
    partial = mm(hidden, w_mlp, ((1,), (1,)))
    result = middle + (partial[:rows] + swap(partial[rows:].astype(BF)))
    layer_output = give_back(result.astype(BF))

    grad_hidden = mm(cot_all, w_mlp)
    slope = phi + gate * (jnp.exp(-0.5 * gate * gate) * (2.0 * jnp.pi) ** -0.5)
    grad_gate = (grad_hidden * up * slope).astype(BF)
    grad_up = (grad_hidden * act).astype(BF)
    d_mlp = mm(cot_all, hidden, ((0,), (0,))).astype(BF)
    d_gate = mm(low_two, grad_gate, ((0,), (0,))).astype(BF)
    d_up = mm(low_two, grad_up, ((0,), (0,))).astype(BF)
    partial = mm(grad_gate, w_gate, ((1,), (1,))) + mm(grad_up, w_up, ((1,), (1,)))
    grad_two = partial[:rows] + swap(partial[rows:].astype(BF))
    back, gain_two_grad = norm_back(grad_two, gain_two, norm_two, scale_two)
    grad_middle = cot.astype(F32) + back
    branch = grad_middle.astype(BF)
    d_out_own = mm(att_own, branch, ((0,), (0,)))
    d_out_far = mm(att_far, branch, ((0,), (0,)))
    d_out = jnp.where(
        c == 0, jnp.concatenate([d_out_own, d_out_far]), jnp.concatenate([d_out_far, d_out_own])
    ).reshape(width, 2, half_width)
    d_out_mine = lax.dynamic_index_in_dim(d_out, c, 1, keepdims=False)
    d_out_theirs = lax.dynamic_index_in_dim(d_out, 1 - c, 1, keepdims=False)
    d_out = (d_out_mine + swap(d_out_theirs.astype(BF))).astype(BF)
    ga_own = mm(branch, w_out_own, ((1,), (1,))).astype(BF)
    ga_far = swap(mm(branch, w_out_far, ((1,), (1,))).astype(BF))
    grad_att = jnp.concatenate([ga_own, ga_far], 0).reshape(2 * rows, HEADS // 2, HEAD_DIM)
    gq, gk, gv = attend_back(q, k, v, lse, grad_att, seq_ids)
    gpair = jnp.stack([gq, gk], axis=1).astype(F32)
    gpair = gpair * cosine + turn_back(gpair * sine)
    grad_proj = jnp.concatenate([gpair.astype(BF), gv[:, None]], axis=1).reshape(2 * rows, -1)
    d_qkv = mm(low_one, grad_proj, ((0,), (0,))).astype(BF)
    partial = mm(grad_proj, w_qkv, ((1,), (1,)))
    grad_one = partial[:rows] + swap(partial[rows:].astype(BF))
    back, gain_one_grad = norm_back(grad_one, gain_one, norm_one, scale_one)
    input_grad = give_back((grad_middle + back).astype(BF))

    def reduce(d):
        d = lax.psum_scatter(d, ("q", "sp"), scatter_dimension=0, tiled=True)
        d = lax.all_gather(d, "sp", axis=0, tiled=True).reshape(2, shard, -1)
        own = lax.dynamic_index_in_dim(d, c, 0, keepdims=False)
        far = swap(lax.dynamic_index_in_dim(d, 1 - c, 0, keepdims=False))
        return own, far

    def joined(d, parts):
        own, far = (x.astype(F32).reshape(shard, parts, 1, -1) for x in reduce(d))
        both = jnp.where(
            c == 0, jnp.concatenate([own, far], 2), jnp.concatenate([far, own], 2)
        )
        return both.reshape(shard, -1)

    mlp_grad = joined(d_mlp, 1).T
    input_grad_w = jnp.concatenate([joined(d_gate, 1), joined(d_up, 1)], 1)
    out_grad = joined(d_out, 1)
    qkv_grad = joined(d_qkv, 3)
    gain_grads = lax.psum(jnp.stack([gain_one_grad, gain_two_grad]), ("sp", "q", "core"))
    at = (2 * lax.axis_index("q") + c) * shard
    gain_grads = lax.dynamic_slice_in_dim(gain_grads, at, shard, 1)
    return (
        layer_output,
        input_grad,
        qkv_grad,
        out_grad,
        input_grad_w,
        mlp_grad,
        gain_grads[0],
        gain_grads[1],
    )


def solution(mesh):
    sp_count, fsdp_count = mesh.devices.shape
    split = Mesh(mesh.devices.reshape(sp_count, fsdp_count // 2, 2), ("sp", "q", "core"))
    fsdp = ("q", "core")
    big = P(None, fsdp, "sp", None)
    return jax.shard_map(
        on_device,
        mesh=split,
        in_specs=(
            big,
            big,
            P(None, fsdp, "sp"),
            P(None, fsdp, None),
            P(fsdp, None),
            P(fsdp, None),
            P(fsdp, None),
            P(None, fsdp),
            P(fsdp),
            P(fsdp),
        ),
        out_specs=(
            big,
            big,
            P(fsdp, None),
            P(fsdp, None),
            P(fsdp, None),
            P(None, fsdp),
            P(fsdp),
            P(fsdp),
        ),
        check_vma=False,
    )
```

```python
import functools

import jax
import jax.numpy as jnp
from jax import lax
from jax.experimental import pallas as pl
from jax.experimental.pallas import tpu as pltpu
from jax.sharding import Mesh, PartitionSpec as P

HEADS = 16
HEAD_DIM = 64
norm_epsilon = 1e-05
rotary_base = 160000.0
masked_score = -1e30
BF = jnp.bfloat16
F32 = jnp.float32
SWAP = [(0, 1), (1, 0)]


def mm(a, b, dims=((1,), (0,))):
    return lax.dot_general(a, b, (dims, ((), ())), preferred_element_type=F32)


def swap(x):
    return lax.ppermute(x, "core", SWAP)


def norm_parts(values):
    centre = values - jnp.mean(values, axis=-1, keepdims=True)
    spread = jnp.mean(centre * centre, axis=-1, keepdims=True)
    scale = lax.rsqrt(spread + norm_epsilon)
    return centre * scale, scale


def norm_back(grad, gain, n, scale):
    h = grad * gain
    back = scale * (
        h - jnp.mean(h, axis=-1, keepdims=True) - n * jnp.mean(h * n, axis=-1, keepdims=True)
    )
    return back, jnp.sum(grad * n, axis=0)


def rotary_tables(places):
    exponents = jnp.arange(0, HEAD_DIM, 2).astype(F32) / HEAD_DIM
    inverse_freq = 1.0 / rotary_base**exponents
    angles = places.astype(F32)[:, None] * jnp.tile(inverse_freq, 128 // (HEAD_DIM // 2))[None, :]
    lane = jnp.arange(128) % HEAD_DIM
    sine = jnp.sin(angles)
    return jnp.cos(angles), jnp.where(lane[None, :] < HEAD_DIM // 2, -sine, sine)


def sequence_layout(lengths_row, positions):
    seq_ends = jnp.cumsum(lengths_row)
    passed = (positions[:, None] >= seq_ends[None, :]).astype(jnp.int32)
    seq_ids = jnp.sum(passed, axis=1)
    seq_starts = jnp.sum(passed * lengths_row[None, :], axis=1)
    return seq_ids, positions - seq_starts, seq_starts


def hop(x, bit):
    n = lax.axis_size("sp")
    return lax.ppermute(x, "sp", [(i, i ^ bit) for i in range(n)])


def along(x):
    n = lax.axis_size("q")
    return lax.ppermute(x, "q", [(i, (i + 1) % n) for i in range(n)])


def at_index(x, i, axis):
    return lax.dynamic_index_in_dim(x, i, axis, keepdims=False)


def spread(x, bits):
    s = lax.axis_index("sp")
    one = hop(x, bits[0])
    two = hop(jnp.stack([x, one]), bits[1])
    full = jnp.zeros((4,) + x.shape, x.dtype)
    for block, mask in ((x, 0), (one, bits[0]), (two[0], bits[1]), (two[1], 3)):
        full = lax.dynamic_update_index_in_dim(full, block, s ^ mask, 0)
    return full


def gather_rows(parts, token=None):
    n, q = lax.axis_size("q"), lax.axis_index("q")
    if n > 8:
        return [lax.all_gather(x, ("q", "sp"), axis=0, tiled=True) for x in parts]
    widths = [-x.shape[1] % 128 for x in parts]
    x = jnp.concatenate([jnp.pad(x, ((0, 0), (0, w))) for x, w in zip(parts, widths)], axis=1)
    near = jnp.zeros((n,) + x.shape, x.dtype)
    near = lax.dynamic_update_index_in_dim(near, x, q, 0)
    moving = x
    for step in range(1, n):
        moving = along(moving)
        near = lax.dynamic_update_index_in_dim(near, moving, (q - step) % n, 0)
    out, at = [], 0
    for j, (p, w) in enumerate(zip(parts, widths)):
        cols = p.shape[1]
        full = spread(near[:, :, at : at + cols], (1, 2) if j % 2 == 0 else (2, 1))
        out.append(full.transpose(1, 0, 2, 3).reshape(-1, cols))
        at += cols + w
    return out


def reduce_rows(terms):
    n, q, s = lax.axis_size("q"), lax.axis_index("q"), lax.axis_index("sp")
    if n > 8:
        return [
            lax.psum_scatter(x, ("q", "sp"), scatter_dimension=0, tiled=True) for x in terms
        ]
    y, z = s // 2, s % 2
    quarter = []
    for j, x in enumerate(terms):
        x = x.reshape(n, 2, 2, -1, x.shape[1])
        steps = ((2, z, 1), (1, y, 2)) if j % 2 == 0 else ((1, y, 2), (1, z, 1))
        for axis, own, bit in steps:
            away = hop(at_index(x, 1 - own, axis).astype(BF), bit)
            x = at_index(x, own, axis).astype(F32) + away.astype(F32)
        quarter.append(jnp.pad(x, ((0, 0), (0, 0), (0, -x.shape[2] % 128))))
    x = jnp.concatenate(quarter, axis=2)
    moving = at_index(x, (q - 1) % n, 0)
    for step in range(1, n):
        got = along(moving.astype(BF)).astype(F32)
        moving = at_index(x, (q - step - 1) % n, 0) + got
    out, at = [], 0
    for term, part in zip(terms, quarter):
        out.append(moving[:, at : at + term.shape[1]].astype(BF))
        at += part.shape[2]
    return out


def exchange_kernel(back, staged, *refs):
    n = lax.axis_size("q")
    s, q, c = lax.axis_index("sp"), lax.axis_index("q"), lax.axis_index("core")
    count = (len(refs) - 4 - staged) // 2
    sources, targets = refs[:count], refs[count : 2 * count]
    send, recv, local, *stages = refs[2 * count :]
    stages, stage_sem = stages[:-1], stages[-1]
    half, odd = s // 2, s % 2
    far = [(ds, dq) for dq in range(n) for ds in range(4)]
    near = [(dt * 2 + dc, dq) for dq in range(n) for dt in range(2) for dc in range(2)]

    def dealt(j):
        ds, dq = far[j]
        return (s ^ ds, lax.rem(q + dq, n), half)

    def held(j):
        d, dq = near[j]
        t, core = odd ^ (d // 2), c ^ (d % 2)
        return (2 * c + t, lax.rem(q + dq, n), core)

    def dealt_slot(ref, place):
        return ref.at[place[1], place[0]]

    def held_slot(ref, place):
        return ref.at[lax.rem(place[0], 2), place[2], place[1]]

    out_place, in_place = (held, dealt) if back else (dealt, held)
    out_slot, in_slot = (held_slot, dealt_slot) if back else (dealt_slot, held_slot)
    me = (s, q, c)
    mine_is_local = c == half

    def remote(a, j):
        return pltpu.make_async_remote_copy(
            src_ref=out_slot(sources[a], out_place(j)),
            dst_ref=in_slot(targets[a], me),
            send_sem=send.at[a, j],
            recv_sem=in_slot(recv.at[a], me),
            device_id=out_place(j),
            device_id_type=pl.DeviceIdType.MESH,
        )

    def arriving(a, j):
        return pltpu.make_async_remote_copy(
            src_ref=in_slot(targets[a], in_place(j)),
            dst_ref=in_slot(targets[a], in_place(j)),
            send_sem=send.at[a, j],
            recv_sem=in_slot(recv.at[a], in_place(j)),
            device_id=in_place(j),
            device_id_type=pl.DeviceIdType.MESH,
        )

    for j in range(1, len(far)):
        for a in range(count):
            remote(a, j).start()

    @pl.when(jnp.logical_not(mine_is_local))
    def _():
        for a in range(count):
            remote(a, 0).start()

    @pl.when(mine_is_local)
    def _():
        for a in range(count):
            take = pltpu.make_async_copy(out_slot(sources[a], me), stages[a], stage_sem.at[a])
            take.start()
            take.wait()
            put = pltpu.make_async_copy(stages[a], in_slot(targets[a], me), local.at[a])
            put.start()
            put.wait()

    @pl.when(jnp.logical_not(mine_is_local))
    def _():
        for a in range(count):
            remote(a, 0).wait_send()
            arriving(a, 0).wait_recv()

    for j in range(1, len(far)):
        for a in range(count):
            remote(a, j).wait_send()
            arriving(a, j).wait_recv()


def exchange(arrays, back):
    n = lax.axis_size("q")
    count = len(arrays)
    lead = (n, 4) if back else (2, 2, n)
    skip = 3 if back else 2
    slots = (n, 4) if back else (2, 2, n)
    shapes = [jax.ShapeDtypeStruct(lead + x.shape[skip:], x.dtype) for x in arrays]
    return pl.pallas_call(
        functools.partial(exchange_kernel, back, count),
        out_shape=shapes,
        in_specs=[pl.BlockSpec(memory_space=pl.ANY)] * count,
        out_specs=[pl.BlockSpec(memory_space=pl.ANY)] * count,
        scratch_shapes=[
            pltpu.SemaphoreType.DMA((count, 4 * n)),
            pltpu.SemaphoreType.DMA((count,) + slots),
            pltpu.SemaphoreType.DMA((count,)),
        ]
        + [pltpu.VMEM(x.shape[skip:], x.dtype) for x in arrays]
        + [pltpu.SemaphoreType.DMA((count,))],
        compiler_params=pltpu.CompilerParams(has_side_effects=True),
        name="give_back" if back else "deal",
    )(*arrays)


def load_kernel(n, x_ref, note_ref, pa_ref, pb_ref, x_out, note_out, wa_out, wb_out, *scratch):
    send, recv, z_send, z_recv, y_send, y_recv, local, xs, ns, ws_a, ws_b = scratch
    s, q, c = lax.axis_index("sp"), lax.axis_index("q"), lax.axis_index("core")
    half, odd = s // 2, s % 2
    pieces, fulls, stages = (pa_ref, pb_ref), (wa_out, wb_out), (ws_a, ws_b)
    rows = ((x_ref, x_out, xs), (note_ref, note_out, ns))

    def remote(src, dst, one, two, place):
        return pltpu.make_async_remote_copy(
            src_ref=src, dst_ref=dst, send_sem=one, recv_sem=two,
            device_id=place, device_id_type=pl.DeviceIdType.MESH,
        )

    def along_z(a, dq):
        return remote(
            pieces[a], fulls[a].at[q, s], z_send.at[a, dq], z_recv.at[a, q],
            (s, lax.rem(q + dq, n), c),
        )

    def from_z(a, dq):
        other = lax.rem(q + dq, n)
        slot = fulls[a].at[other, s]
        return remote(slot, slot, z_send.at[a, dq], z_recv.at[a, other], (s, other, c))

    def in_plane(a, dq, d):
        block = lax.rem(q + dq, n)
        slot = fulls[a].at[block, s]
        src = pieces[a] if dq == 0 else slot
        return remote(src, slot, y_send.at[a, dq, d], y_recv.at[a, block, s], (s ^ d, q, c))

    def from_plane(a, dq, d):
        block = lax.rem(q + dq, n)
        slot = fulls[a].at[block, s ^ d]
        return remote(slot, slot, y_send.at[a, dq, d], y_recv.at[a, block, s ^ d], (s ^ d, q, c))

    def deal(a, ds, dq):
        src, dst, _ = rows[a]
        to_s, to_q = s ^ ds, lax.rem(q + dq, n)
        return remote(
            src.at[to_q, to_s], dst.at[odd, c, q], send.at[a, ds, dq], recv.at[a, odd, c, q],
            (to_s, to_q, half),
        )

    def dealt(a, d, dq):
        t, core, block = odd ^ (d // 2), c ^ (d % 2), lax.rem(q + dq, n)
        slot = rows[a][1].at[t, core, block]
        return remote(
            slot, slot, send.at[a, d, dq], recv.at[a, t, core, block], (2 * c + t, block, core)
        )

    def stay(src, mid, dst, sem):
        take = pltpu.make_async_copy(src, mid, sem)
        take.start()
        take.wait()
        put = pltpu.make_async_copy(mid, dst, sem)
        put.start()
        put.wait()

    others = [(d, dq) for dq in range(n) for d in range(4) if d or dq]
    for a in range(2):
        for dq in range(1, n):
            along_z(a, dq).start()
    for a in range(2):
        for d in range(1, 4):
            in_plane(a, 0, d).start()
    for d, dq in others:
        for a in range(2):
            deal(a, d, dq).start()

    @pl.when(c != half)
    def _():
        for a in range(2):
            deal(a, 0, 0).start()

    @pl.when(c == half)
    def _():
        for a, (src, dst, mid) in enumerate(rows):
            stay(src.at[q, s], mid, dst.at[odd, c, q], local.at[a])

    for a in range(2):
        stay(pieces[a], stages[a], fulls[a].at[q, s], local.at[2 + a])
    for dq in range(1, n):
        for a in range(2):
            along_z(a, dq).wait_send()
            from_z(a, dq).wait_recv()
            for d in range(1, 4):
                in_plane(a, dq, d).start()

    @pl.when(c != half)
    def _():
        for a in range(2):
            deal(a, 0, 0).wait_send()
            dealt(a, 0, 0).wait_recv()

    for d, dq in others:
        for a in range(2):
            deal(a, d, dq).wait_send()
            dealt(a, d, dq).wait_recv()
    for dq in range(n):
        for a in range(2):
            for d in range(1, 4):
                in_plane(a, dq, d).wait_send()
                from_plane(a, dq, d).wait_recv()


def load(rows, note, pa, pb):
    n = lax.axis_size("q")
    lead = (2, 2, n)
    dma = pltpu.SemaphoreType.DMA
    return pl.pallas_call(
        functools.partial(load_kernel, n),
        out_shape=[
            jax.ShapeDtypeStruct(lead + rows.shape[2:], rows.dtype),
            jax.ShapeDtypeStruct(lead + note.shape[2:], note.dtype),
            jax.ShapeDtypeStruct((n, 4) + pa.shape, pa.dtype),
            jax.ShapeDtypeStruct((n, 4) + pb.shape, pb.dtype),
        ],
        in_specs=[pl.BlockSpec(memory_space=pl.ANY)] * 4,
        out_specs=[pl.BlockSpec(memory_space=pl.ANY)] * 4,
        scratch_shapes=[
            dma((2, 4, n)),
            dma((2, 2, 2, n)),
            dma((2, n)),
            dma((2, n)),
            dma((2, n, 4)),
            dma((2, n, 4)),
            dma((4,)),
            pltpu.VMEM(rows.shape[2:], rows.dtype),
            pltpu.VMEM(note.shape[2:], note.dtype),
            pltpu.VMEM(pa.shape, pa.dtype),
            pltpu.VMEM(pb.shape, pb.dtype),
        ],
        compiler_params=pltpu.CompilerParams(has_side_effects=True),
        name="load",
    )(rows, note, pa, pb)


BLK = 256


def lane_halves(shape):
    return lax.broadcasted_iota(jnp.int32, shape, len(shape) - 1) < HEAD_DIM


def turned(u, sine):
    lane = lax.broadcasted_iota(jnp.int32, u.shape, 1) % HEAD_DIM
    half = HEAD_DIM // 2
    swapped = jnp.where(lane < half, pltpu.roll(u, 128 - half, 1), pltpu.roll(u, half, 1))
    return swapped * sine


def project_kernel(x_ref, wa_ref, wb_ref, cos_ref, sin_ref, out_ref):
    cols = wa_ref.shape[1] // 3
    cosine, sine = cos_ref[...], sin_ref[...]
    for j in range(6):
        w_ref = wa_ref if j < 3 else wb_ref
        acc = mm(x_ref[...], w_ref[:, j % 3 * cols : (j % 3 + 1) * cols])
        for at in range(0, cols, 128):
            u = acc[:, at : at + 128]
            if j < 4:
                u = u * cosine + turned(u, sine)
            if j < 2:
                u = u.astype(BF).astype(F32) * HEAD_DIM**-0.5
            here = j % 2 * cols + at
            out_ref[j // 2, :, here : here + 128] = u.astype(BF)


def project(x, wa, wb, cosine, sine):
    rows, width = x.shape
    cols = wa.shape[1] // 3 * 2
    fixed = pl.BlockSpec(wa.shape, lambda i: (0, 0))
    return pl.pallas_call(
        project_kernel,
        out_shape=jax.ShapeDtypeStruct((3, rows, cols), BF),
        grid=(rows // BLK,),
        in_specs=[
            pl.BlockSpec((BLK, width), lambda i: (i, 0)),
            fixed,
            fixed,
            pl.BlockSpec((BLK, 128), lambda i: (i, 0)),
            pl.BlockSpec((BLK, 128), lambda i: (i, 0)),
        ],
        out_specs=pl.BlockSpec((3, BLK, cols), lambda i: (0, i, 0)),
        cost_estimate=pl.CostEstimate(
            flops=6 * rows * width * cols, bytes_accessed=16 * rows * cols, transcendentals=0
        ),
        name="project",
    )(x, wa, wb, cosine, sine)


def attend_kernel(lim_ref, q_ref, k_ref, v_ref, idc_ref, idr_ref, o_ref, lse_ref, s_ref, m_ref, l_ref, a_ref):
    i = pl.program_id(1)
    blocks = k_ref.shape[0] // BLK
    low, high, shift = lim_ref[i, 0], lim_ref[i, 1], lim_ref[i, 2]
    first = lane_halves((BLK, 128))
    zero = jnp.zeros((BLK, 128), BF)
    q = q_ref[...]
    q_of = (jnp.where(first, q, zero), jnp.where(first, zero, q))
    ids = idc_ref[:, :1]
    m_ref[...] = jnp.full_like(m_ref, masked_score)
    l_ref[...] = jnp.zeros_like(l_ref)
    a_ref[...] = jnp.zeros_like(a_ref)

    @pl.loop(low, high)
    def _(kb):
        at = lax.rem(kb + shift, blocks)
        keys = k_ref[pl.ds(pl.multiple_of(at * BLK, BLK), BLK), :]
        same = ids == idr_ref[at, :1, :]
        for h in range(2):
            sc = jnp.where(same, mm(q_of[h], keys, ((1,), (1,))), masked_score)
            s_ref[h, kb] = sc
            m_ref[h] = jnp.maximum(m_ref[h], jnp.maximum(sc[:, :128], sc[:, 128:]))

    tops = [jnp.max(m_ref[h], axis=1, keepdims=True) for h in range(2)]

    @pl.loop(low, high)
    def _(kb):
        at = lax.rem(kb + shift, blocks)
        vals = v_ref[pl.ds(pl.multiple_of(at * BLK, BLK), BLK), :]
        for h in range(2):
            p = jnp.exp(s_ref[h, kb] - tops[h])
            l_ref[h] = l_ref[h] + (p[:, :128] + p[:, 128:])
            a_ref[h] = a_ref[h] + mm(p.astype(BF), vals)

    sums = [jnp.sum(l_ref[h], axis=1, keepdims=True) for h in range(2)]
    o_ref[...] = jnp.where(first, a_ref[0] / sums[0], a_ref[1] / sums[1]).astype(BF)
    logs = [tops[h] + jnp.log(sums[h]) for h in range(2)]
    lse_ref[...] = jnp.where(first, logs[0], logs[1])


def attend(qkv, limits, id_col, id_row):
    _, rows, cols = qkv.shape
    blocks = rows // BLK
    whole = lambda part: pl.BlockSpec((pl.squeezed, rows, 128), lambda p, i, _: (part, 0, p))
    tile = pl.BlockSpec((BLK, 128), lambda p, i, _: (i, p))
    return pl.pallas_call(
        attend_kernel,
        out_shape=(
            jax.ShapeDtypeStruct((rows, cols), BF),
            jax.ShapeDtypeStruct((rows, cols), F32),
        ),
        grid_spec=pltpu.PrefetchScalarGridSpec(
            num_scalar_prefetch=1,
            grid=(cols // 128, blocks),
            in_specs=[
                pl.BlockSpec((pl.squeezed, BLK, 128), lambda p, i, _: (0, i, p)),
                whole(1),
                whole(2),
                pl.BlockSpec((BLK, 128), lambda p, i, _: (i, 0)),
                pl.BlockSpec((blocks, 8, BLK), lambda p, i, _: (0, 0, 0)),
            ],
            out_specs=[tile, tile],
            scratch_shapes=[
                pltpu.VMEM((2, blocks, BLK, BLK), F32),
                pltpu.VMEM((2, BLK, 128), F32),
                pltpu.VMEM((2, BLK, 128), F32),
                pltpu.VMEM((2, BLK, 128), F32),
            ],
        ),
        cost_estimate=pl.CostEstimate(
            flops=4 * rows * rows * cols, bytes_accessed=8 * rows * cols, transcendentals=rows * rows * 8
        ),
        name="attend",
    )(limits, qkv, qkv, qkv, id_col, id_row)


def attend_back_kernel(
    lim_ref, q_ref, k_ref, v_ref, do_ref, o_ref, lse_ref, idc_ref, idr_ref, cos_ref, sin_ref,
    out_ref, dk_ref, dv_ref, dq_ref
):
    i = pl.program_id(1)
    blocks = k_ref.shape[0] // BLK
    low, high, shift = lim_ref[i, 0], lim_ref[i, 1], lim_ref[i, 2]

    @pl.when(i == 0)
    def _():
        dk_ref[...] = jnp.zeros_like(dk_ref)
        dv_ref[...] = jnp.zeros_like(dv_ref)

    dq_ref[...] = jnp.zeros_like(dq_ref)
    first = lane_halves((BLK, 128))
    zero = jnp.zeros((BLK, 128), BF)
    q, do = q_ref[...], do_ref[...]
    q_of = (jnp.where(first, q, zero), jnp.where(first, zero, q))
    do_of = (jnp.where(first, do, zero), jnp.where(first, zero, do))
    lse = lse_ref[...].T
    lse_of = (lse[:1], lse[HEAD_DIM : HEAD_DIM + 1])
    prod = (do.astype(F32) * o_ref[...].astype(F32)).T
    delta_of = (
        jnp.sum(prod[:HEAD_DIM], axis=0, keepdims=True),
        jnp.sum(prod[HEAD_DIM:], axis=0, keepdims=True),
    )
    ids = idr_ref[i, :1, :]

    @pl.loop(low, high)
    def _(kb):
        at = lax.rem(kb + shift, blocks)
        here = pl.ds(pl.multiple_of(at * BLK, BLK), BLK)
        keys, vals = k_ref[here, :], v_ref[here, :]
        same = idc_ref[here, :1] == ids
        k_of = (jnp.where(first, keys, zero), jnp.where(first, zero, keys))
        dk = dv = dq = None
        for h in range(2):
            sc = jnp.where(same, mm(keys, q_of[h], ((1,), (1,))) - lse_of[h], masked_score)
            p = jnp.exp(sc)
            gp = mm(vals, do_of[h], ((1,), (1,)))
            gs = (p * (gp - delta_of[h])).astype(BF)
            a, b, d = mm(gs, q_of[h]), mm(p.astype(BF), do_of[h]), mm(gs, k_of[h], ((0,), (0,)))
            dk, dv, dq = (a, b, d) if h == 0 else (dk + a, dv + b, dq + d)
        dk_ref[here, :] = dk_ref[here, :] + dk
        dv_ref[here, :] = dv_ref[here, :] + dv
        dq_ref[...] = dq_ref[...] + dq

    def back(g, cosine, sine):
        g = g.astype(BF).astype(F32)
        return (g * cosine - turned(g, sine)).astype(BF)

    mine = pl.ds(pl.multiple_of(i * BLK, BLK), BLK)
    out_ref[0, mine, :] = back(dq_ref[...] * HEAD_DIM**-0.5, cos_ref[mine, :], sin_ref[mine, :])

    @pl.when(i == blocks - 1)
    def _():
        for j in range(blocks):
            cut = slice(j * BLK, (j + 1) * BLK)
            out_ref[1, cut, :] = back(dk_ref[cut, :], cos_ref[cut, :], sin_ref[cut, :])
            out_ref[2, cut, :] = dv_ref[cut, :].astype(BF)


def attend_back(qkv, grad, out, lse, limits, id_col, id_row, cosine, sine, base, pairs):
    _, rows, cols = qkv.shape
    blocks = rows // BLK
    whole = lambda part: pl.BlockSpec((pl.squeezed, rows, 128), lambda p, i, _: (part, 0, p + base))
    tile = pl.BlockSpec((BLK, 128), lambda p, i, _: (i, p + base))
    fixed = pl.BlockSpec((rows, 128), lambda p, i, _: (0, 0))
    return pl.pallas_call(
        attend_back_kernel,
        out_shape=jax.ShapeDtypeStruct((3, rows, pairs * 128), BF),
        grid_spec=pltpu.PrefetchScalarGridSpec(
            num_scalar_prefetch=1,
            grid=(pairs, blocks),
            in_specs=[
                pl.BlockSpec((pl.squeezed, BLK, 128), lambda p, i, _: (0, i, p + base)),
                whole(1),
                whole(2),
                tile,
                tile,
                tile,
                fixed,
                pl.BlockSpec((blocks, 8, BLK), lambda p, i, _: (0, 0, 0)),
                fixed,
                fixed,
            ],
            out_specs=pl.BlockSpec((3, rows, 128), lambda p, i, _: (0, 0, p)),
            scratch_shapes=[
                pltpu.VMEM((rows, 128), F32),
                pltpu.VMEM((rows, 128), F32),
                pltpu.VMEM((BLK, 128), F32),
            ],
        ),
        cost_estimate=pl.CostEstimate(
            flops=1280 * rows * rows * pairs,
            bytes_accessed=2560 * rows * pairs,
            transcendentals=2 * rows * rows * pairs,
        ),
        name="attend_back",
    )(limits, qkv, qkv, qkv, grad, out, lse, id_col, id_row, cosine, sine)


def on_device(
    tokens,
    cotangent,
    destination,
    seq_lengths,
    qkv_weight,
    output_weight,
    input_weight,
    mlp_weight,
    first_gain,
    second_gain,
):
    sp_count, q_count = lax.axis_size("sp"), lax.axis_size("q")
    s, c = lax.axis_index("sp"), lax.axis_index("core")
    batches, _, block, width = tokens.shape
    groups = 2 * q_count
    each = block // groups
    shard = qkv_weight.shape[0]
    part = 2 * shard // sp_count
    half_ff = mlp_weight.shape[0] // 2
    half_width = width // 2
    rows = 2 * block

    owner = s // (sp_count // 2)
    first_row = (s % (sp_count // 2)) * part

    def cut_rows(w, parts):
        w = lax.dynamic_slice_in_dim(w, first_row, part, 0)
        cols = w.shape[1] // (2 * parts)
        blocks = [w[:, j * cols : (j + 1) * cols] for j in range(2 * parts)]
        return blocks[0::2], blocks[1::2]

    cuts = [
        cut_rows(qkv_weight, 3),
        cut_rows(output_weight, 1),
        cut_rows(input_weight, 2),
        cut_rows(mlp_weight.T, 1),
    ]

    def piece(k):
        return [
            jnp.concatenate([jnp.where(k == 0, x, y) for x, y in zip(*pair)], 1) for pair in cuts[:2]
        ] + [
            jnp.concatenate(
                [
                    jnp.pad(jnp.where(k == 0, x, y), ((0, 0), (0, -x.shape[1] % 128)))
                    for pair in (cuts[3], cuts[2])
                    for x, y in zip(*pair)
                ],
                1,
            )
        ]

    mine, theirs = piece(c), piece(1 - c)
    is_owner = c == owner
    p_qkv, p_out, p_ffn = [jnp.where(is_owner, a, swap(b)) for a, b in zip(mine, theirs)]
    cut = p_qkv.shape[1] // 2
    rest = jnp.concatenate([p_out, p_ffn], 1)
    rest = lax.all_gather(rest, ("q", "sp"), axis=0, tiled=True)
    dest = destination[:, 0]
    group_of, slot_of = dest // block, dest % block
    idx = jnp.arange(block, dtype=jnp.int32)
    before = (group_of[:, :, None] == group_of[:, None, :]) & (idx[None, None, :] < idx[None, :, None])
    place = group_of * each + jnp.sum(before.astype(jnp.int32), axis=-1)
    picks = idx[None, :, None] == place[:, None, :]
    sort_low = picks.astype(BF)
    slots = jnp.sum(jnp.where(picks, slot_of[:, None, :], 0), axis=-1)
    my_batch, my_pair = s // 2, s % 2

    def by_owner(x):
        x = x.reshape((batches, q_count, 2) + x.shape[2:]).swapaxes(0, 1)
        return x.reshape((q_count, sp_count) + x.shape[3:])

    def lanes(x):
        return jnp.pad(x.astype(F32), [(0, 0)] * (x.ndim - 1) + [(0, 128 - x.shape[-1])])

    note_shape = (batches, groups, 128)
    note = jnp.stack(
        [
            jnp.broadcast_to(lanes(first_gain), note_shape),
            jnp.broadcast_to(lanes(second_gain), note_shape),
            lanes(slots.reshape(batches, groups, each)),
            jnp.broadcast_to(lanes(seq_lengths[:, 0])[:, None], note_shape),
        ],
        axis=2,
    )
    note = by_owner(jnp.pad(note, ((0, 0), (0, 0), (0, 4), (0, 0))))

    def sort_rows(x):
        x = jnp.einsum("bij,bjd->bid", sort_low, x[:, 0], preferred_element_type=F32).astype(BF)
        return by_owner(x.reshape(batches, groups, each, width))

    rows_in = sort_rows(tokens)
    if part % 16 == 0:
        got_rows, notes, w_qkv_a, w_qkv_b = load(
            rows_in, note, p_qkv[:, :cut], p_qkv[:, cut:]
        )
        w_qkv_a, w_qkv_b = w_qkv_a.reshape(width, cut), w_qkv_b.reshape(width, cut)
    else:
        got_rows, notes = exchange([rows_in, note], False)
        w_qkv_a, w_qkv_b = gather_rows([p_qkv[:, :cut], p_qkv[:, cut:]])
    gains = notes[0, :, :, :2, :shard].transpose(2, 1, 0, 3).reshape(2, width)
    gain_one, gain_two = gains[0], gains[1]
    my_slots = notes[:, :, :, 2, :each].reshape(2, block).astype(jnp.int32)
    my_note = lax.dynamic_index_in_dim(notes[0], my_pair, 0, keepdims=False)
    my_note = lax.dynamic_index_in_dim(my_note, lax.axis_index("q"), 0, keepdims=False)
    lengths_row = my_note[3, : seq_lengths.shape[2]].astype(jnp.int32)
    place_low = (idx[None, :, None] == my_slots[:, None, :]).astype(BF)
    def deal_plane(got):
        got = lax.all_to_all(got, "sp", 1, 0, tiled=True)
        got = got.reshape(2, 2, q_count, each, width)
        own = lax.dynamic_index_in_dim(got, c, 0, keepdims=False)
        far = swap(lax.dynamic_index_in_dim(got, 1 - c, 0, keepdims=False))
        both = jnp.stack([jnp.where(c == 0, own, far), jnp.where(c == 0, far, own)], axis=1)
        both = both.reshape(2, block, width)
        return jnp.einsum("tri,tid->trd", place_low, both, preferred_element_type=F32).reshape(
            rows, width
        )

    def back_plane(x):
        x = x.reshape(2, block, width)
        x = jnp.einsum("tri,trd->tid", place_low, x, preferred_element_type=F32).astype(BF)
        x = x.reshape(2, 2, q_count, each, width)
        own = lax.dynamic_index_in_dim(x, c, 1, keepdims=False)
        far = swap(lax.dynamic_index_in_dim(x, 1 - c, 1, keepdims=False))
        both = jnp.where(c == 0, jnp.stack([own, far]), jnp.stack([far, own]))
        both = both.reshape(sp_count, q_count, each, width)
        return lax.all_to_all(both, "sp", 0, 0, tiled=True)

    def back_line(got):
        got = got.reshape(sp_count, q_count, each, width).transpose(1, 0, 2, 3)
        return lax.all_to_all(got, "q", 0, 0, tiled=True)

    def unsort(got):
        got = got.reshape(q_count, batches, 2, each, width).transpose(1, 0, 2, 3, 4)
        got = got.reshape(batches, block, width)
        out = jnp.einsum("bij,bid->bjd", sort_low, got, preferred_element_type=F32)
        return out.astype(BF)[:, None]

    cot_rows, got_rows = lax.optimization_barrier((sort_rows(cotangent), got_rows))
    cot_rows = lax.all_to_all(cot_rows, "q", 0, 0, tiled=True)
    owned = jnp.einsum(
        "tri,tid->trd", place_low, got_rows.reshape(2, block, width), preferred_element_type=F32
    ).reshape(rows, width)
    positions = (c * rows + jnp.arange(2 * rows, dtype=jnp.int32)) % (2 * rows)
    seq_ids, places, starts = sequence_layout(lengths_row, positions)
    cosine, sine = rotary_tables(places)
    blocks = 2 * rows // BLK
    seq_of_row = jnp.arange(lengths_row.shape[0])[None, :] == seq_ids[:, None]
    ends = starts + jnp.sum(jnp.where(seq_of_row, lengths_row[None, :], 0), axis=1)
    low = starts[::BLK] // BLK
    high = (ends[BLK - 1 :: BLK] + BLK - 1) // BLK
    limits = jnp.stack([low, high, jnp.full_like(low, c * (blocks // 2))], axis=1).astype(jnp.int32)
    id_col = jnp.broadcast_to(seq_ids[:, None], (2 * rows, 128))
    id_row = jnp.broadcast_to(seq_ids.reshape(blocks, 1, BLK), (blocks, 8, BLK))

    norm_one, scale_one = norm_parts(owned)
    low_one = (norm_one * gain_one).astype(BF)
    low_one = jnp.concatenate([low_one, swap(low_one)], 0)
    qkv = project(low_one, w_qkv_a, w_qkv_b, cosine, sine)
    att, lse = attend(qkv, limits, id_col, id_row)
    rest, att, cot_rows = lax.optimization_barrier((rest, att, cot_rows))
    w_out_half = rest[:, :half_width]
    ffn_step = (rest.shape[1] - half_width) // 3
    w_mlp, w_gate, w_up = (
        rest[:, half_width + j * ffn_step : half_width + j * ffn_step + half_ff] for j in range(3)
    )
    w_out_other = swap(w_out_half)
    w_out = jnp.where(
        c == 0,
        jnp.concatenate([w_out_half, w_out_other], 1),
        jnp.concatenate([w_out_other, w_out_half], 1),
    )
    w_out_rows = w_out.reshape(2, half_width, width)
    w_out_own = lax.dynamic_index_in_dim(w_out_rows, c, 0, keepdims=False)
    w_out_far = lax.dynamic_index_in_dim(w_out_rows, 1 - c, 0, keepdims=False)

    cot = deal_plane(cot_rows).astype(BF)
    att_own, att_far = att[:rows], swap(att[rows:])
    middle = owned + (mm(att_own, w_out_own) + mm(att_far, w_out_far))
    norm_two, scale_two = norm_parts(middle)
    low_two = (norm_two * gain_two).astype(BF)
    low_two = jnp.concatenate([low_two, swap(low_two)], 0)
    cot_all = jnp.concatenate([cot, swap(cot)], 0)
    gate, up = mm(low_two, w_gate), mm(low_two, w_up)
    phi = 0.5 * (1.0 + lax.erf(gate * (0.5**0.5)))
    act = gate * phi
    hidden = (act * up).astype(BF)
    partial = mm(hidden, w_mlp, ((1,), (1,)))
    result = middle + (partial[:rows] + swap(partial[rows:].astype(BF)))
    result_rows = back_plane(result.astype(BF))

    grad_hidden = mm(cot_all, w_mlp)
    slope = phi + gate * (jnp.exp(-0.5 * gate * gate) * (2.0 * jnp.pi) ** -0.5)
    grad_gate = (grad_hidden * up * slope).astype(BF)
    grad_up = (grad_hidden * act).astype(BF)
    d_mlp = mm(cot_all, hidden, ((0,), (0,))).astype(BF)
    d_gate = mm(low_two, grad_gate, ((0,), (0,))).astype(BF)
    d_up = mm(low_two, grad_up, ((0,), (0,))).astype(BF)
    partial = mm(grad_gate, w_gate, ((1,), (1,))) + mm(grad_up, w_up, ((1,), (1,)))
    grad_two = partial[:rows] + swap(partial[rows:].astype(BF))
    result_rows, grad_two = lax.optimization_barrier((result_rows, grad_two))
    result_rows = back_line(result_rows)
    back, gain_two_grad = norm_back(grad_two, gain_two, norm_two, scale_two)
    grad_middle = cot.astype(F32) + back
    branch = grad_middle.astype(BF)
    d_out_own = mm(att_own, branch, ((0,), (0,)))
    d_out_far = mm(att_far, branch, ((0,), (0,)))
    d_out = jnp.where(
        c == 0, jnp.concatenate([d_out_own, d_out_far]), jnp.concatenate([d_out_far, d_out_own])
    ).reshape(width, 2, half_width)
    d_out_mine = lax.dynamic_index_in_dim(d_out, c, 1, keepdims=False)
    d_out_theirs = lax.dynamic_index_in_dim(d_out, 1 - c, 1, keepdims=False)
    d_out = (d_out_mine + swap(d_out_theirs.astype(BF))).astype(BF)
    ga_own = mm(branch, w_out_own, ((1,), (1,))).astype(BF)
    ga_far = swap(mm(branch, w_out_far, ((1,), (1,))).astype(BF))
    grad_att = jnp.concatenate([ga_own, ga_far], 0)
    pairs = half_width // 256
    halves = [
        attend_back(
            qkv, grad_att, att, lse, limits, id_col, id_row, cosine, sine, j * pairs, pairs
        )
        for j in range(2)
    ]
    layer_output, halves = lax.optimization_barrier((result_rows, halves))
    layer_output = unsort(layer_output)
    pieces = [halves[j % 2][j // 2] for j in range(6)]
    grad_a, grad_b = jnp.concatenate(pieces[:3], 1), jnp.concatenate(pieces[3:], 1)
    d_qkv_a = mm(low_one, grad_a, ((0,), (0,))).astype(BF)
    d_qkv_b = mm(low_one, grad_b, ((0,), (0,))).astype(BF)
    partial = mm(grad_a, w_qkv_a, ((1,), (1,))) + mm(grad_b, w_qkv_b, ((1,), (1,)))
    grad_one = partial[:rows] + swap(partial[rows:].astype(BF))
    back, gain_one_grad = norm_back(grad_one, gain_one, norm_one, scale_one)
    x = (grad_middle + back).astype(BF).reshape(2, block, width)
    x = jnp.einsum("tri,trd->tid", place_low, x, preferred_element_type=F32).astype(BF)
    (x,) = exchange([x.reshape(2, 2, q_count, each, width)], True)
    input_grad = unsort(x)

    def finish(terms):
        summed = reduce_rows(terms)
        out = []
        for j, d in enumerate(summed):
            if q_count > 8:
                d = lax.all_gather(d, "sp", axis=0)
            else:
                d = spread(d, (1, 2) if j % 2 == 0 else (2, 1))
            d = d.reshape(2, shard, -1)
            own = lax.dynamic_index_in_dim(d, c, 0, keepdims=False)
            far = swap(lax.dynamic_index_in_dim(d, 1 - c, 0, keepdims=False))
            out.append((own, far))
        return out

    def joined(own, far):
        return jnp.where(c == 0, own, far), jnp.where(c == 0, far, own)

    wide = jnp.concatenate(
        [jnp.pad(x, ((0, 0), (0, -x.shape[1] % 128))) for x in (d_mlp, d_gate, d_up)], 1
    )
    wide = lax.psum_scatter(wide, ("q", "sp"), scatter_dimension=0, tiled=True)
    wide = lax.all_gather(wide, "sp", axis=0, tiled=True).reshape(2, shard, -1)
    own = lax.dynamic_index_in_dim(wide, c, 0, keepdims=False)
    far = swap(lax.dynamic_index_in_dim(wide, 1 - c, 0, keepdims=False))
    step = wide.shape[2] // 3
    low, high = joined(own, far)
    r_mlp, r_gate, r_up = (
        [x[:, j * step : j * step + half_ff] for x in (low, high)] for j in range(3)
    )
    gain_terms = jnp.pad(jnp.stack([gain_one_grad, gain_two_grad], 1), ((0, 0), (0, 126)))
    r_out, r_qkv_a, r_qkv_b, r_gain = finish(
        [d_out, d_qkv_a, d_qkv_b, gain_terms.astype(BF)]
    )
    mlp_grad = jnp.concatenate(r_mlp, 1).T.astype(F32)
    input_grad_w = jnp.concatenate(r_gate + r_up, 1).astype(F32)
    out_grad = jnp.concatenate(joined(*r_out), 1).astype(F32)
    qa, qb = joined(*r_qkv_a), joined(*r_qkv_b)
    third, half = qa[0].shape[1] // 3 * 2, qa[0].shape[1] // 3
    qkv_grad = jnp.concatenate(
        [qa[0][:, :third], qa[1][:, :third]]
        + [qa[0][:, third:], qb[0][:, :half], qa[1][:, third:], qb[1][:, :half]]
        + [qb[0][:, half:], qb[1][:, half:]],
        1,
    ).astype(F32)
    gain_grads = (r_gain[0].astype(F32) + r_gain[1].astype(F32)).T
    return (
        layer_output,
        input_grad,
        qkv_grad,
        out_grad,
        input_grad_w,
        mlp_grad,
        gain_grads[0],
        gain_grads[1],
    )


def solution(mesh):
    sp_count, fsdp_count = mesh.devices.shape
    split = Mesh(mesh.devices.reshape(sp_count, fsdp_count // 2, 2), ("sp", "q", "core"))
    fsdp = ("q", "core")
    big = P(None, fsdp, "sp", None)
    return jax.shard_map(
        on_device,
        mesh=split,
        in_specs=(
            big,
            big,
            P(None, fsdp, "sp"),
            P(None, fsdp, None),
            P(fsdp, None),
            P(fsdp, None),
            P(fsdp, None),
            P(None, fsdp),
            P(fsdp),
            P(fsdp),
        ),
        out_specs=(
            big,
            big,
            P(fsdp, None),
            P(fsdp, None),
            P(fsdp, None),
            P(None, fsdp),
            P(fsdp),
            P(fsdp),
        ),
        check_vma=False,
    )
```

```python
import functools
import math

import jax
import jax.numpy as jnp
from jax import lax
from jax.experimental import pallas as pl
from jax.experimental.pallas import tpu as pltpu
from jax.sharding import Mesh, PartitionSpec as P

HEADS = 16
HEAD_DIM = 64
norm_epsilon = 1e-05
rotary_base = 160000.0
masked_score = -1e30
BF = jnp.bfloat16
F32 = jnp.float32
SWAP = [(0, 1), (1, 0)]


def mm(a, b, dims=((1,), (0,))):
    return lax.dot_general(a, b, (dims, ((), ())), preferred_element_type=F32)


def swap(x):
    return lax.ppermute(x, "core", SWAP)


def norm_parts(values):
    centre = values - jnp.mean(values, axis=-1, keepdims=True)
    spread = jnp.mean(centre * centre, axis=-1, keepdims=True)
    scale = lax.rsqrt(spread + norm_epsilon)
    return centre * scale, scale


def norm_back(grad, gain, n, scale):
    h = grad * gain
    back = scale * (
        h - jnp.mean(h, axis=-1, keepdims=True) - n * jnp.mean(h * n, axis=-1, keepdims=True)
    )
    return back, jnp.sum(grad * n, axis=0)


def rotary_tables(places):
    exponents = jnp.arange(0, HEAD_DIM, 2).astype(F32) / HEAD_DIM
    inverse_freq = 1.0 / rotary_base**exponents
    angles = places.astype(F32)[:, None] * jnp.tile(inverse_freq, 128 // (HEAD_DIM // 2))[None, :]
    lane = jnp.arange(128) % HEAD_DIM
    sine = jnp.sin(angles)
    return jnp.cos(angles), jnp.where(lane[None, :] < HEAD_DIM // 2, -sine, sine)


def sequence_layout(lengths_row, positions):
    seq_ends = jnp.cumsum(lengths_row)
    passed = (positions[:, None] >= seq_ends[None, :]).astype(jnp.int32)
    seq_ids = jnp.sum(passed, axis=1)
    seq_starts = jnp.sum(passed * lengths_row[None, :], axis=1)
    return seq_ids, positions - seq_starts, seq_starts


def hop(x, bit):
    n = lax.axis_size("sp")
    return lax.ppermute(x, "sp", [(i, i ^ bit) for i in range(n)])


def along(x):
    n = lax.axis_size("q")
    return lax.ppermute(x, "q", [(i, (i + 1) % n) for i in range(n)])


def at_index(x, i, axis):
    return lax.dynamic_index_in_dim(x, i, axis, keepdims=False)


def spread(x, bits):
    s = lax.axis_index("sp")
    one = hop(x, bits[0])
    two = hop(jnp.stack([x, one]), bits[1])
    full = jnp.zeros((4,) + x.shape, x.dtype)
    for block, mask in ((x, 0), (one, bits[0]), (two[0], bits[1]), (two[1], 3)):
        full = lax.dynamic_update_index_in_dim(full, block, s ^ mask, 0)
    return full


def gather_rows(parts, token=None):
    n, q = lax.axis_size("q"), lax.axis_index("q")
    if n > 8:
        return [lax.all_gather(x, ("q", "sp"), axis=0, tiled=True) for x in parts]
    widths = [-x.shape[1] % 128 for x in parts]
    x = jnp.concatenate([jnp.pad(x, ((0, 0), (0, w))) for x, w in zip(parts, widths)], axis=1)
    near = jnp.zeros((n,) + x.shape, x.dtype)
    near = lax.dynamic_update_index_in_dim(near, x, q, 0)
    moving = x
    for step in range(1, n):
        moving = along(moving)
        near = lax.dynamic_update_index_in_dim(near, moving, (q - step) % n, 0)
    out, at = [], 0
    for j, (p, w) in enumerate(zip(parts, widths)):
        cols = p.shape[1]
        full = spread(near[:, :, at : at + cols], (1, 2) if j % 2 == 0 else (2, 1))
        out.append(full.transpose(1, 0, 2, 3).reshape(-1, cols))
        at += cols + w
    return out


def reduce_rows(terms, after):
    n, q, s = lax.axis_size("q"), lax.axis_index("q"), lax.axis_index("sp")
    if n > 8:
        return [
            lax.psum_scatter(x, ("q", "sp"), scatter_dimension=0, tiled=True) for x in terms
        ], after
    y, z = s // 2, s % 2
    quarter = []
    for j, x in enumerate(terms):
        x = x.reshape(n, 2, 2, -1, x.shape[1])
        steps = ((2, z, 1), (1, y, 2)) if j % 2 == 0 else ((1, y, 2), (1, z, 1))
        for axis, own, bit in steps:
            away = hop(at_index(x, 1 - own, axis).astype(BF), bit)
            x = at_index(x, own, axis).astype(F32) + away.astype(F32)
        quarter.append(jnp.pad(x, ((0, 0), (0, 0), (0, -x.shape[2] % 128))))
    quarter, after = lax.optimization_barrier((quarter, after))
    x = jnp.concatenate(quarter, axis=2)
    moving = at_index(x, (q - 1) % n, 0)
    for step in range(1, n):
        got = along(moving.astype(BF)).astype(F32)
        moving = at_index(x, (q - step - 1) % n, 0) + got
    out, at = [], 0
    for term, part in zip(terms, quarter):
        out.append(moving[:, at : at + term.shape[1]].astype(BF))
        at += part.shape[2]
    return out, after


def exchange_kernel(back, staged, *refs):
    n = lax.axis_size("q")
    s, q, c = lax.axis_index("sp"), lax.axis_index("q"), lax.axis_index("core")
    count = (len(refs) - 4 - staged) // 2
    sources, targets = refs[:count], refs[count : 2 * count]
    send, recv, local, *stages = refs[2 * count :]
    stages, stage_sem = stages[:-1], stages[-1]
    half, odd = s // 2, s % 2
    far = [(ds, dq) for dq in range(n) for ds in range(4)]
    near = [(dt * 2 + dc, dq) for dq in range(n) for dt in range(2) for dc in range(2)]

    def dealt(j):
        ds, dq = far[j]
        return (s ^ ds, lax.rem(q + dq, n), half)

    def held(j):
        d, dq = near[j]
        t, core = odd ^ (d // 2), c ^ (d % 2)
        return (2 * c + t, lax.rem(q + dq, n), core)

    def dealt_slot(ref, place):
        return ref.at[place[1], place[0]]

    def held_slot(ref, place):
        return ref.at[lax.rem(place[0], 2), place[2], place[1]]

    out_place, in_place = (held, dealt) if back else (dealt, held)
    out_slot, in_slot = (held_slot, dealt_slot) if back else (dealt_slot, held_slot)
    me = (s, q, c)
    mine_is_local = c == half

    def remote(a, j):
        return pltpu.make_async_remote_copy(
            src_ref=out_slot(sources[a], out_place(j)),
            dst_ref=in_slot(targets[a], me),
            send_sem=send.at[a, j],
            recv_sem=in_slot(recv.at[a], me),
            device_id=out_place(j),
            device_id_type=pl.DeviceIdType.MESH,
        )

    def arriving(a, j):
        return pltpu.make_async_remote_copy(
            src_ref=in_slot(targets[a], in_place(j)),
            dst_ref=in_slot(targets[a], in_place(j)),
            send_sem=send.at[a, j],
            recv_sem=in_slot(recv.at[a], in_place(j)),
            device_id=in_place(j),
            device_id_type=pl.DeviceIdType.MESH,
        )

    for j in range(1, len(far)):
        for a in range(count):
            remote(a, j).start()

    @pl.when(jnp.logical_not(mine_is_local))
    def _():
        for a in range(count):
            remote(a, 0).start()

    @pl.when(mine_is_local)
    def _():
        for a in range(count):
            take = pltpu.make_async_copy(out_slot(sources[a], me), stages[a], stage_sem.at[a])
            take.start()
            take.wait()
            put = pltpu.make_async_copy(stages[a], in_slot(targets[a], me), local.at[a])
            put.start()
            put.wait()

    @pl.when(jnp.logical_not(mine_is_local))
    def _():
        for a in range(count):
            remote(a, 0).wait_send()
            arriving(a, 0).wait_recv()

    for j in range(1, len(far)):
        for a in range(count):
            remote(a, j).wait_send()
            arriving(a, j).wait_recv()


def exchange(arrays, back):
    n = lax.axis_size("q")
    count = len(arrays)
    lead = (n, 4) if back else (2, 2, n)
    skip = 3 if back else 2
    slots = (n, 4) if back else (2, 2, n)
    shapes = [jax.ShapeDtypeStruct(lead + x.shape[skip:], x.dtype) for x in arrays]
    return pl.pallas_call(
        functools.partial(exchange_kernel, back, count),
        out_shape=shapes,
        in_specs=[pl.BlockSpec(memory_space=pl.ANY)] * count,
        out_specs=[pl.BlockSpec(memory_space=pl.ANY)] * count,
        scratch_shapes=[
            pltpu.SemaphoreType.DMA((count, 4 * n)),
            pltpu.SemaphoreType.DMA((count,) + slots),
            pltpu.SemaphoreType.DMA((count,)),
        ]
        + [pltpu.VMEM(x.shape[skip:], x.dtype) for x in arrays]
        + [pltpu.SemaphoreType.DMA((count,))],
        compiler_params=pltpu.CompilerParams(has_side_effects=True),
        cost_estimate=pl.CostEstimate(
            flops=20_000_000_000, bytes_accessed=10_000_000, transcendentals=0
        ),
        name="give_back" if back else "deal",
    )(*arrays)


def load_kernel(n, x_ref, note_ref, pa_ref, pb_ref, x_out, note_out, wa_out, wb_out, *scratch):
    send, recv, z_send, z_recv, y_send, y_recv, local, xs, ns, ws_a, ws_b = scratch
    s, q, c = lax.axis_index("sp"), lax.axis_index("q"), lax.axis_index("core")
    half, odd = s // 2, s % 2
    pieces, fulls, stages = (pa_ref, pb_ref), (wa_out, wb_out), (ws_a, ws_b)
    rows = ((x_ref, x_out, xs), (note_ref, note_out, ns))

    def remote(src, dst, one, two, place):
        return pltpu.make_async_remote_copy(
            src_ref=src, dst_ref=dst, send_sem=one, recv_sem=two,
            device_id=place, device_id_type=pl.DeviceIdType.MESH,
        )

    def along_z(a, dq):
        return remote(
            pieces[a], fulls[a].at[q, s], z_send.at[a, dq], z_recv.at[a, q],
            (s, lax.rem(q + dq, n), c),
        )

    def from_z(a, dq):
        other = lax.rem(q + dq, n)
        slot = fulls[a].at[other, s]
        return remote(slot, slot, z_send.at[a, dq], z_recv.at[a, other], (s, other, c))

    def in_plane(a, dq, d):
        block = lax.rem(q + dq, n)
        slot = fulls[a].at[block, s]
        src = pieces[a] if dq == 0 else slot
        return remote(src, slot, y_send.at[a, dq, d], y_recv.at[a, block, s], (s ^ d, q, c))

    def from_plane(a, dq, d):
        block = lax.rem(q + dq, n)
        slot = fulls[a].at[block, s ^ d]
        return remote(slot, slot, y_send.at[a, dq, d], y_recv.at[a, block, s ^ d], (s ^ d, q, c))

    def deal(a, ds, dq):
        src, dst, _ = rows[a]
        to_s, to_q = s ^ ds, lax.rem(q + dq, n)
        return remote(
            src.at[to_q, to_s], dst.at[odd, c, q], send.at[a, ds, dq], recv.at[a, odd, c, q],
            (to_s, to_q, half),
        )

    def dealt(a, d, dq):
        t, core, block = odd ^ (d // 2), c ^ (d % 2), lax.rem(q + dq, n)
        slot = rows[a][1].at[t, core, block]
        return remote(
            slot, slot, send.at[a, d, dq], recv.at[a, t, core, block], (2 * c + t, block, core)
        )

    def stay(src, mid, dst, sem):
        take = pltpu.make_async_copy(src, mid, sem)
        take.start()
        take.wait()
        put = pltpu.make_async_copy(mid, dst, sem)
        put.start()
        put.wait()

    others = [(d, dq) for dq in range(n) for d in range(4) if d or dq]
    for a in range(2):
        for dq in range(1, n):
            along_z(a, dq).start()
    for a in range(2):
        for d in range(1, 4):
            in_plane(a, 0, d).start()
    for d, dq in others:
        for a in range(2):
            deal(a, d, dq).start()

    @pl.when(c != half)
    def _():
        for a in range(2):
            deal(a, 0, 0).start()

    @pl.when(c == half)
    def _():
        for a, (src, dst, mid) in enumerate(rows):
            stay(src.at[q, s], mid, dst.at[odd, c, q], local.at[a])

    for a in range(2):
        stay(pieces[a], stages[a], fulls[a].at[q, s], local.at[2 + a])
    for dq in range(1, n):
        for a in range(2):
            along_z(a, dq).wait_send()
            from_z(a, dq).wait_recv()
            for d in range(1, 4):
                in_plane(a, dq, d).start()

    @pl.when(c != half)
    def _():
        for a in range(2):
            deal(a, 0, 0).wait_send()
            dealt(a, 0, 0).wait_recv()

    for d, dq in others:
        for a in range(2):
            deal(a, d, dq).wait_send()
            dealt(a, d, dq).wait_recv()
    for dq in range(n):
        for a in range(2):
            for d in range(1, 4):
                in_plane(a, dq, d).wait_send()
                from_plane(a, dq, d).wait_recv()


def load(rows, note, pa, pb):
    n = lax.axis_size("q")
    lead = (2, 2, n)
    dma = pltpu.SemaphoreType.DMA
    return pl.pallas_call(
        functools.partial(load_kernel, n),
        out_shape=[
            jax.ShapeDtypeStruct(lead + rows.shape[2:], rows.dtype),
            jax.ShapeDtypeStruct(lead + note.shape[2:], note.dtype),
            jax.ShapeDtypeStruct((n, 4) + pa.shape, pa.dtype),
            jax.ShapeDtypeStruct((n, 4) + pb.shape, pb.dtype),
        ],
        in_specs=[pl.BlockSpec(memory_space=pl.ANY)] * 4,
        out_specs=[pl.BlockSpec(memory_space=pl.ANY)] * 4,
        scratch_shapes=[
            dma((2, 4, n)),
            dma((2, 2, 2, n)),
            dma((2, n)),
            dma((2, n)),
            dma((2, n, 4)),
            dma((2, n, 4)),
            dma((4,)),
            pltpu.VMEM(rows.shape[2:], rows.dtype),
            pltpu.VMEM(note.shape[2:], note.dtype),
            pltpu.VMEM(pa.shape, pa.dtype),
            pltpu.VMEM(pb.shape, pb.dtype),
        ],
        compiler_params=pltpu.CompilerParams(has_side_effects=True),
        cost_estimate=pl.CostEstimate(
            flops=20_000_000_000, bytes_accessed=10_000_000, transcendentals=0
        ),
        name="load",
    )(rows, note, pa, pb)


BLK = 256
FWD = 512
BACK = 256


def lane_halves(shape):
    return lax.broadcasted_iota(jnp.int32, shape, len(shape) - 1) < HEAD_DIM


def turned(u, sine):
    lane = lax.broadcasted_iota(jnp.int32, u.shape, 1) % HEAD_DIM
    half = HEAD_DIM // 2
    swapped = jnp.where(lane < half, pltpu.roll(u, 128 - half, 1), pltpu.roll(u, half, 1))
    return swapped * sine


def project_kernel(x_ref, wa_ref, wb_ref, cos_ref, sin_ref, out_ref):
    cols = wa_ref.shape[1] // 3
    cosine, sine = cos_ref[...], sin_ref[...]
    for j in range(6):
        w_ref = wa_ref if j < 3 else wb_ref
        acc = mm(x_ref[...], w_ref[:, j % 3 * cols : (j % 3 + 1) * cols])
        for at in range(0, cols, 128):
            u = acc[:, at : at + 128]
            if j < 4:
                u = u * cosine + turned(u, sine)
            if j < 2:
                u = u.astype(BF).astype(F32) * HEAD_DIM**-0.5
            here = j % 2 * cols + at
            out_ref[j // 2, :, here : here + 128] = u.astype(BF)


def project(x, wa, wb, cosine, sine):
    rows, width = x.shape
    cols = wa.shape[1] // 3 * 2
    fixed = pl.BlockSpec(wa.shape, lambda i: (0, 0))
    return pl.pallas_call(
        project_kernel,
        out_shape=jax.ShapeDtypeStruct((3, rows, cols), BF),
        grid=(rows // BLK,),
        in_specs=[
            pl.BlockSpec((BLK, width), lambda i: (i, 0)),
            fixed,
            fixed,
            pl.BlockSpec((BLK, 128), lambda i: (i, 0)),
            pl.BlockSpec((BLK, 128), lambda i: (i, 0)),
        ],
        out_specs=pl.BlockSpec((3, BLK, cols), lambda i: (0, i, 0)),
        cost_estimate=pl.CostEstimate(
            flops=6 * rows * width * cols, bytes_accessed=16 * rows * cols, transcendentals=0
        ),
        name="project",
    )(x, wa, wb, cosine, sine)


def attend_kernel(lim_ref, q_ref, k_ref, v_ref, idc_ref, idr_ref, o_ref, lse_ref, s_ref, m_ref, l_ref, a_ref):
    i = pl.program_id(1)
    blocks = k_ref.shape[0] // BLK
    low, high, shift = lim_ref[i, 0], lim_ref[i, 1], lim_ref[i, 2]
    first = lane_halves((BLK, 128))
    zero = jnp.zeros((BLK, 128), BF)
    tiles = [slice(at, at + 128) for at in range(0, q_ref.shape[1], 128)]
    q_of = []
    for t in tiles:
        q = q_ref[:, t]
        q_of += [jnp.where(first, q, zero), jnp.where(first, zero, q)]
    ids = idc_ref[:, :1]
    m_ref[...] = jnp.full_like(m_ref, masked_score)
    l_ref[...] = jnp.zeros_like(l_ref)
    a_ref[...] = jnp.zeros_like(a_ref)

    @pl.loop(low, high)
    def _(kb):
        at = lax.rem(kb + shift, blocks)
        here = pl.ds(pl.multiple_of(at * BLK, BLK), BLK)
        same = ids == idr_ref[at, :1, :]
        for h, q in enumerate(q_of):
            sc = jnp.where(same, mm(q, k_ref[here, tiles[h // 2]], ((1,), (1,))), masked_score)
            s_ref[h, kb] = sc
            m_ref[h] = jnp.maximum(m_ref[h], jnp.maximum(sc[:, :128], sc[:, 128:]))

    tops = [jnp.max(m_ref[h], axis=1, keepdims=True) for h in range(len(q_of))]

    @pl.loop(low, high)
    def _(kb):
        at = lax.rem(kb + shift, blocks)
        here = pl.ds(pl.multiple_of(at * BLK, BLK), BLK)
        for h in range(len(q_of)):
            p = jnp.exp(s_ref[h, kb] - tops[h])
            l_ref[h] = l_ref[h] + (p[:, :128] + p[:, 128:])
            a_ref[h] = a_ref[h] + mm(p.astype(BF), v_ref[here, tiles[h // 2]])

    for j, t in enumerate(tiles):
        sums = [jnp.sum(l_ref[h], axis=1, keepdims=True) for h in (2 * j, 2 * j + 1)]
        out = jnp.where(first, a_ref[2 * j] / sums[0], a_ref[2 * j + 1] / sums[1])
        o_ref[:, t] = out.astype(BF)
        logs = [tops[2 * j + h] + jnp.log(sums[h]) for h in range(2)]
        lse_ref[:, t] = jnp.where(first, logs[0], logs[1])


def attend(qkv, limits, id_col, id_row):
    _, rows, cols = qkv.shape
    blocks = rows // BLK
    whole = lambda part: pl.BlockSpec((pl.squeezed, rows, FWD), lambda p, i, _: (part, 0, p))
    tile = pl.BlockSpec((BLK, FWD), lambda p, i, _: (i, p))
    heads = FWD // HEAD_DIM
    return pl.pallas_call(
        attend_kernel,
        out_shape=(
            jax.ShapeDtypeStruct((rows, cols), BF),
            jax.ShapeDtypeStruct((rows, cols), F32),
        ),
        grid_spec=pltpu.PrefetchScalarGridSpec(
            num_scalar_prefetch=1,
            grid=(cols // FWD, blocks),
            in_specs=[
                pl.BlockSpec((pl.squeezed, BLK, FWD), lambda p, i, _: (0, i, p)),
                whole(1),
                whole(2),
                pl.BlockSpec((BLK, 128), lambda p, i, _: (i, 0)),
                pl.BlockSpec((blocks, 8, BLK), lambda p, i, _: (0, 0, 0)),
            ],
            out_specs=[tile, tile],
            scratch_shapes=[
                pltpu.VMEM((heads, blocks, BLK, BLK), F32),
                pltpu.VMEM((heads, BLK, 128), F32),
                pltpu.VMEM((heads, BLK, 128), F32),
                pltpu.VMEM((heads, BLK, 128), F32),
            ],
        ),
        cost_estimate=pl.CostEstimate(
            flops=4 * rows * rows * cols, bytes_accessed=8 * rows * cols, transcendentals=rows * rows * 8
        ),
        name="attend",
    )(limits, qkv, qkv, qkv, id_col, id_row)


def attend_back_kernel(
    lim_ref, q_ref, k_ref, v_ref, do_ref, o_ref, lse_ref, idc_ref, idr_ref, cos_ref, sin_ref,
    out_ref, dk_ref, dv_ref, dq_ref
):
    i = pl.program_id(1)
    blocks = k_ref.shape[0] // BLK
    low, high, shift = lim_ref[i, 0], lim_ref[i, 1], lim_ref[i, 2]

    @pl.when(i == 0)
    def _():
        dk_ref[...] = jnp.zeros_like(dk_ref)
        dv_ref[...] = jnp.zeros_like(dv_ref)

    dq_ref[...] = jnp.zeros_like(dq_ref)
    first = lane_halves((BLK, 128))
    zero = jnp.zeros((BLK, 128), BF)
    tiles = [slice(at, at + 128) for at in range(0, q_ref.shape[1], 128)]
    q_of, do_of, lse_of, delta_of = [], [], [], []
    for t in tiles:
        q, do = q_ref[:, t], do_ref[:, t]
        q_of += [jnp.where(first, q, zero), jnp.where(first, zero, q)]
        do_of += [jnp.where(first, do, zero), jnp.where(first, zero, do)]
        lse = lse_ref[:, t].T
        lse_of += [lse[:1], lse[HEAD_DIM : HEAD_DIM + 1]]
        prod = (do.astype(F32) * o_ref[:, t].astype(F32)).T
        delta_of += [
            jnp.sum(prod[:HEAD_DIM], axis=0, keepdims=True),
            jnp.sum(prod[HEAD_DIM:], axis=0, keepdims=True),
        ]
    ids = idr_ref[i, :1, :]

    @pl.loop(low, high)
    def _(kb):
        at = lax.rem(kb + shift, blocks)
        here = pl.ds(pl.multiple_of(at * BLK, BLK), BLK)
        same = idc_ref[here, :1] == ids
        for j, t in enumerate(tiles):
            keys, vals = k_ref[here, t], v_ref[here, t]
            k_of = (jnp.where(first, keys, zero), jnp.where(first, zero, keys))
            scores, probs = [], []
            for h in (2 * j, 2 * j + 1):
                sc = mm(keys, q_of[h], ((1,), (1,))) - lse_of[h]
                p = jnp.exp(jnp.where(same, sc, masked_score))
                gp = mm(vals, do_of[h], ((1,), (1,)))
                scores.append((p * (gp - delta_of[h])).astype(BF))
                probs.append(p.astype(BF))
            pair = slice(2 * j, 2 * j + 2)
            gs, ps = jnp.concatenate(scores, 1), jnp.concatenate(probs, 1)
            dk_ref[here, t] += mm(gs, jnp.concatenate(q_of[pair], 0))
            dv_ref[here, t] += mm(ps, jnp.concatenate(do_of[pair], 0))
            dq_ref[:, t] += mm(
                jnp.concatenate(scores, 0), jnp.concatenate(k_of, 0), ((0,), (0,))
            )

    def back(g, cosine, sine):
        g = g.astype(BF).astype(F32)
        return (g * cosine - turned(g, sine)).astype(BF)

    mine = pl.ds(pl.multiple_of(i * BLK, BLK), BLK)
    for t in tiles:
        out_ref[0, mine, t] = back(dq_ref[:, t] * HEAD_DIM**-0.5, cos_ref[mine, :], sin_ref[mine, :])

    @pl.when(i == blocks - 1)
    def _():
        for t in tiles:
            for j in range(blocks):
                cut = slice(j * BLK, (j + 1) * BLK)
                out_ref[1, cut, t] = back(dk_ref[cut, t], cos_ref[cut, :], sin_ref[cut, :])
                out_ref[2, cut, t] = dv_ref[cut, t].astype(BF)


def attend_back(qkv, grad, out, lse, limits, id_col, id_row, cosine, sine, base, pairs):
    _, rows, cols = qkv.shape
    blocks = rows // BLK
    base, steps = base * 128 // BACK, pairs * 128 // BACK
    whole = lambda part: pl.BlockSpec((pl.squeezed, rows, BACK), lambda p, i, _: (part, 0, p + base))
    tile = pl.BlockSpec((BLK, BACK), lambda p, i, _: (i, p + base))
    fixed = pl.BlockSpec((rows, 128), lambda p, i, _: (0, 0))
    return pl.pallas_call(
        attend_back_kernel,
        out_shape=jax.ShapeDtypeStruct((3, rows, pairs * 128), BF),
        grid_spec=pltpu.PrefetchScalarGridSpec(
            num_scalar_prefetch=1,
            grid=(steps, blocks),
            in_specs=[
                pl.BlockSpec((pl.squeezed, BLK, BACK), lambda p, i, _: (0, i, p + base)),
                whole(1),
                whole(2),
                tile,
                tile,
                tile,
                fixed,
                pl.BlockSpec((blocks, 8, BLK), lambda p, i, _: (0, 0, 0)),
                fixed,
                fixed,
            ],
            out_specs=pl.BlockSpec((3, rows, BACK), lambda p, i, _: (0, 0, p)),
            scratch_shapes=[
                pltpu.VMEM((rows, BACK), F32),
                pltpu.VMEM((rows, BACK), F32),
                pltpu.VMEM((BLK, BACK), F32),
            ],
        ),
        cost_estimate=pl.CostEstimate(
            flops=1280 * rows * rows * pairs,
            bytes_accessed=2560 * rows * pairs,
            transcendentals=2 * rows * rows * pairs,
        ),
        name="attend_back",
    )(limits, qkv, qkv, qkv, grad, out, lse, id_col, id_row, cosine, sine)


def ffn_kernel(lead, step, x_ref, y_ref, w_ref, hidden_ref, gate_ref, up_ref):
    x, y = x_ref[...], y_ref[...]
    for at in range(0, step, 256):
        n = min(256, step - at)
        grad = mm(y, w_ref[:, lead + at : lead + at + n])
        gate = mm(x, w_ref[:, lead + step + at : lead + step + at + n])
        up = mm(x, w_ref[:, lead + 2 * step + at : lead + 2 * step + at + n])
        phi = 0.5 + 0.5 * lax.erf(gate * 0.5**0.5)
        slope = phi + gate * (jnp.exp(gate * gate * -0.5) * (2.0 * math.pi) ** -0.5)
        act = gate * phi
        hidden_ref[:, at : at + n] = (act * up).astype(BF)
        gate_ref[:, at : at + n] = (grad * up * slope).astype(BF)
        up_ref[:, at : at + n] = (grad * act).astype(BF)


def ffn(x, y, w, lead, step):
    rows, width = x.shape
    tall = rows // 3
    tile = pl.BlockSpec((tall, width), lambda i: (i, 0))
    out = pl.BlockSpec((tall, step), lambda i: (i, 0))
    return pl.pallas_call(
        functools.partial(ffn_kernel, lead, step),
        out_shape=[jax.ShapeDtypeStruct((rows, step), BF)] * 3,
        grid=(3,),
        in_specs=[tile, tile, pl.BlockSpec(w.shape, lambda i: (0, 0), pipeline_mode=pl.Buffered(1))],
        out_specs=[out] * 3,
        cost_estimate=pl.CostEstimate(
            flops=6 * rows * width * step,
            bytes_accessed=2 * width * w.shape[1] + 4 * rows * width + 6 * rows * step,
            transcendentals=2 * rows * step,
        ),
        name="ffn",
    )(x, y, w)


def ffn_weights_kernel(step, y_ref, x_ref, hidden_ref, gate_ref, up_ref, out_ref, turn_ref):
    turn_ref[0] = y_ref[...].T
    turn_ref[1] = x_ref[...].T
    for j, ref in enumerate((hidden_ref, gate_ref, up_ref)):
        for at in range(0, step, 256):
            n = min(256, step - at)
            got = mm(turn_ref[min(j, 1)], ref[:, at : at + n])
            out_ref[:, j * step + at : j * step + at + n] = got.astype(BF)


def ffn_weights(y, x, hidden, gate, up):
    rows, width = x.shape
    step, wide = hidden.shape[1], width // 2
    tile = pl.BlockSpec((rows, wide), lambda i: (0, i))
    whole = pl.BlockSpec((rows, step), lambda i: (0, 0), pipeline_mode=pl.Buffered(1))
    return pl.pallas_call(
        functools.partial(ffn_weights_kernel, step),
        out_shape=jax.ShapeDtypeStruct((width, 3 * step), BF),
        grid=(2,),
        in_specs=[tile, tile, whole, whole, whole],
        out_specs=pl.BlockSpec((wide, 3 * step), lambda i: (i, 0)),
        scratch_shapes=[pltpu.VMEM((2, wide, rows), BF)],
        cost_estimate=pl.CostEstimate(
            flops=6 * rows * width * step,
            bytes_accessed=4 * rows * width + 6 * rows * step + 6 * width * step,
            transcendentals=0,
        ),
        name="ffn_weights",
    )(y, x, hidden, gate, up)


def on_device(
    tokens,
    cotangent,
    destination,
    seq_lengths,
    qkv_weight,
    output_weight,
    input_weight,
    mlp_weight,
    first_gain,
    second_gain,
):
    sp_count, q_count = lax.axis_size("sp"), lax.axis_size("q")
    s, c = lax.axis_index("sp"), lax.axis_index("core")
    batches, _, block, width = tokens.shape
    groups = 2 * q_count
    each = block // groups
    shard = qkv_weight.shape[0]
    part = 2 * shard // sp_count
    half_ff = mlp_weight.shape[0] // 2
    half_width = width // 2
    rows = 2 * block

    owner = s // (sp_count // 2)
    first_row = (s % (sp_count // 2)) * part

    def cut_rows(w, parts):
        w = lax.dynamic_slice_in_dim(w, first_row, part, 0)
        cols = w.shape[1] // (2 * parts)
        blocks = [w[:, j * cols : (j + 1) * cols] for j in range(2 * parts)]
        return blocks[0::2], blocks[1::2]

    cuts = [
        cut_rows(qkv_weight, 3),
        cut_rows(output_weight, 1),
        cut_rows(input_weight, 2),
        cut_rows(mlp_weight.T, 1),
    ]

    def piece(k):
        return [
            jnp.concatenate([jnp.where(k == 0, x, y) for x, y in zip(*pair)], 1) for pair in cuts[:2]
        ] + [
            jnp.concatenate(
                [
                    jnp.pad(jnp.where(k == 0, x, y), ((0, 0), (0, -x.shape[1] % 128)))
                    for pair in (cuts[3], cuts[2])
                    for x, y in zip(*pair)
                ],
                1,
            )
        ]

    mine, theirs = piece(c), piece(1 - c)
    is_owner = c == owner
    p_qkv, p_out, p_ffn = [jnp.where(is_owner, a, swap(b)) for a, b in zip(mine, theirs)]
    cut = p_qkv.shape[1] // 2
    rest = jnp.concatenate([p_out, p_ffn], 1)
    rest = lax.all_gather(rest, ("q", "sp"), axis=0, tiled=True)
    dest = destination[:, 0]
    group_of, slot_of = dest // block, dest % block
    idx = jnp.arange(block, dtype=jnp.int32)
    before = (group_of[:, :, None] == group_of[:, None, :]) & (idx[None, None, :] < idx[None, :, None])
    place = group_of * each + jnp.sum(before.astype(jnp.int32), axis=-1)
    picks = idx[None, :, None] == place[:, None, :]
    sort_low = picks.astype(BF)
    slots = jnp.sum(jnp.where(picks, slot_of[:, None, :], 0), axis=-1)
    my_batch, my_pair = s // 2, s % 2

    def by_owner(x):
        x = x.reshape((batches, q_count, 2) + x.shape[2:]).swapaxes(0, 1)
        return x.reshape((q_count, sp_count) + x.shape[3:])

    def lanes(x):
        return jnp.pad(x.astype(F32), [(0, 0)] * (x.ndim - 1) + [(0, 128 - x.shape[-1])])

    note_shape = (batches, groups, 128)
    note = jnp.stack(
        [
            jnp.broadcast_to(lanes(first_gain), note_shape),
            jnp.broadcast_to(lanes(second_gain), note_shape),
            lanes(slots.reshape(batches, groups, each)),
            jnp.broadcast_to(lanes(seq_lengths[:, 0])[:, None], note_shape),
        ],
        axis=2,
    )
    note = by_owner(jnp.pad(note, ((0, 0), (0, 0), (0, 4), (0, 0))))

    def sort_rows(x):
        x = jnp.einsum("bij,bjd->bid", sort_low, x[:, 0], preferred_element_type=F32).astype(BF)
        return by_owner(x.reshape(batches, groups, each, width))

    rows_in = sort_rows(tokens)
    if part % 16 == 0:
        got_rows, notes, w_qkv_a, w_qkv_b = load(
            rows_in, note, p_qkv[:, :cut], p_qkv[:, cut:]
        )
        w_qkv_a, w_qkv_b = w_qkv_a.reshape(width, cut), w_qkv_b.reshape(width, cut)
    else:
        got_rows, notes = exchange([rows_in, note], False)
        w_qkv_a, w_qkv_b = gather_rows([p_qkv[:, :cut], p_qkv[:, cut:]])
    gains = notes[0, :, :, :2, :shard].transpose(2, 1, 0, 3).reshape(2, width)
    gain_one, gain_two = gains[0], gains[1]
    my_slots = notes[:, :, :, 2, :each].reshape(2, block).astype(jnp.int32)
    my_note = lax.dynamic_index_in_dim(notes[0], my_pair, 0, keepdims=False)
    my_note = lax.dynamic_index_in_dim(my_note, lax.axis_index("q"), 0, keepdims=False)
    lengths_row = my_note[3, : seq_lengths.shape[2]].astype(jnp.int32)
    place_low = (idx[None, :, None] == my_slots[:, None, :]).astype(BF)
    def deal_plane(got):
        got = lax.all_to_all(got, "sp", 1, 0, tiled=True)
        got = got.reshape(2, 2, q_count, each, width)
        own = lax.dynamic_index_in_dim(got, c, 0, keepdims=False)
        far = swap(lax.dynamic_index_in_dim(got, 1 - c, 0, keepdims=False))
        both = jnp.stack([jnp.where(c == 0, own, far), jnp.where(c == 0, far, own)], axis=1)
        both = both.reshape(2, block, width)
        return jnp.einsum("tri,tid->trd", place_low, both, preferred_element_type=F32).reshape(
            rows, width
        )

    def back_plane(x):
        x = x.reshape(2, block, width)
        x = jnp.einsum("tri,trd->tid", place_low, x, preferred_element_type=F32).astype(BF)
        x = x.reshape(2, 2, q_count, each, width)
        own = lax.dynamic_index_in_dim(x, c, 1, keepdims=False)
        far = swap(lax.dynamic_index_in_dim(x, 1 - c, 1, keepdims=False))
        both = jnp.where(c == 0, jnp.stack([own, far]), jnp.stack([far, own]))
        both = both.reshape(sp_count, q_count, each, width)
        return lax.all_to_all(both, "sp", 0, 0, tiled=True)

    def back_line(got):
        got = got.reshape(sp_count, q_count, each, width).transpose(1, 0, 2, 3)
        return lax.all_to_all(got, "q", 0, 0, tiled=True)

    def unsort(got):
        got = got.reshape(q_count, batches, 2, each, width).transpose(1, 0, 2, 3, 4)
        got = got.reshape(batches, block, width)
        out = jnp.einsum("bij,bid->bjd", sort_low, got, preferred_element_type=F32)
        return out.astype(BF)[:, None]

    cot_rows, got_rows = lax.optimization_barrier((sort_rows(cotangent), got_rows))
    cot_rows = lax.all_to_all(cot_rows, "q", 0, 0, tiled=True)
    owned = jnp.einsum(
        "tri,tid->trd", place_low, got_rows.reshape(2, block, width), preferred_element_type=F32
    ).reshape(rows, width)
    positions = (c * rows + jnp.arange(2 * rows, dtype=jnp.int32)) % (2 * rows)
    seq_ids, places, starts = sequence_layout(lengths_row, positions)
    cosine, sine = rotary_tables(places)
    blocks = 2 * rows // BLK
    seq_of_row = jnp.arange(lengths_row.shape[0])[None, :] == seq_ids[:, None]
    ends = starts + jnp.sum(jnp.where(seq_of_row, lengths_row[None, :], 0), axis=1)
    low = starts[::BLK] // BLK
    high = (ends[BLK - 1 :: BLK] + BLK - 1) // BLK
    limits = jnp.stack([low, high, jnp.full_like(low, c * (blocks // 2))], axis=1).astype(jnp.int32)
    id_col = jnp.broadcast_to(seq_ids[:, None], (2 * rows, 128))
    id_row = jnp.broadcast_to(seq_ids.reshape(blocks, 1, BLK), (blocks, 8, BLK))

    norm_one, scale_one = norm_parts(owned)
    low_one = (norm_one * gain_one).astype(BF)
    low_one = jnp.concatenate([low_one, swap(low_one)], 0)
    qkv = project(low_one, w_qkv_a, w_qkv_b, cosine, sine)
    att, lse = attend(qkv, limits, id_col, id_row)
    rest, att, cot_rows = lax.optimization_barrier((rest, att, cot_rows))
    w_out_half = rest[:, :half_width]
    ffn_step = (rest.shape[1] - half_width) // 3
    w_mlp, w_gate, w_up = (
        rest[:, half_width + j * ffn_step : half_width + (j + 1) * ffn_step] for j in range(3)
    )
    w_out_other = swap(w_out_half)
    w_out = jnp.where(
        c == 0,
        jnp.concatenate([w_out_half, w_out_other], 1),
        jnp.concatenate([w_out_other, w_out_half], 1),
    )
    w_out_rows = w_out.reshape(2, half_width, width)
    w_out_own = lax.dynamic_index_in_dim(w_out_rows, c, 0, keepdims=False)
    w_out_far = lax.dynamic_index_in_dim(w_out_rows, 1 - c, 0, keepdims=False)

    cot = deal_plane(cot_rows).astype(BF)
    att_own, att_far = att[:rows], swap(att[rows:])
    middle = owned + (mm(att_own, w_out_own) + mm(att_far, w_out_far))
    norm_two, scale_two = norm_parts(middle)
    low_two = (norm_two * gain_two).astype(BF)
    low_two = jnp.concatenate([low_two, swap(low_two)], 0)
    cot_all = jnp.concatenate([cot, swap(cot)], 0)
    hidden, grad_gate, grad_up = ffn(low_two, cot_all, rest, half_width, ffn_step)
    wide = ffn_weights(cot_all, low_two, hidden, grad_gate, grad_up)
    wide, hidden, grad_gate = lax.optimization_barrier((wide, hidden, grad_gate))
    wide = lax.psum_scatter(wide, ("q", "sp"), scatter_dimension=0, tiled=True)
    partial = mm(hidden, w_mlp, ((1,), (1,)))
    partial, grad_up = lax.optimization_barrier((partial, grad_up))
    result = middle + (partial[:rows] + swap(partial[rows:].astype(BF)))
    result_rows = back_plane(result.astype(BF))

    partial = mm(grad_gate, w_gate, ((1,), (1,))) + mm(grad_up, w_up, ((1,), (1,)))
    grad_two = partial[:rows] + swap(partial[rows:].astype(BF))
    back, gain_two_grad = norm_back(grad_two, gain_two, norm_two, scale_two)
    grad_middle = cot.astype(F32) + back
    branch = grad_middle.astype(BF)
    ga_own = mm(branch, w_out_own, ((1,), (1,))).astype(BF)
    ga_far = swap(mm(branch, w_out_far, ((1,), (1,))).astype(BF))
    grad_att = jnp.concatenate([ga_own, ga_far], 0)
    pairs = half_width // 256
    tables = (limits, id_col, id_row, cosine, sine)
    halves = [attend_back(qkv, grad_att, att, lse, *tables, 0, pairs)]
    result_rows, halves, branch_late, grad_att = lax.optimization_barrier(
        (result_rows, halves, branch, grad_att)
    )
    result_rows = back_line(result_rows)
    d_out_own = mm(att_own, branch_late, ((0,), (0,)))
    d_out_far = mm(att_far, branch_late, ((0,), (0,)))
    d_out = jnp.where(
        c == 0, jnp.concatenate([d_out_own, d_out_far]), jnp.concatenate([d_out_far, d_out_own])
    ).reshape(width, 2, half_width)
    d_out_mine = lax.dynamic_index_in_dim(d_out, c, 1, keepdims=False)
    d_out_theirs = lax.dynamic_index_in_dim(d_out, 1 - c, 1, keepdims=False)
    d_out = (d_out_mine + swap(d_out_theirs.astype(BF))).astype(BF)
    halves = halves + [attend_back(qkv, grad_att, att, lse, *tables, pairs, pairs)]
    pieces = [halves[j % 2][j // 2] for j in range(6)]
    grad_a, grad_b = jnp.concatenate(pieces[:3], 1), jnp.concatenate(pieces[3:], 1)
    d_qkv_a = mm(low_one, grad_a, ((0,), (0,))).astype(BF)
    d_qkv_a, wide = lax.optimization_barrier((d_qkv_a, wide))
    wide = lax.all_gather(wide, "sp", axis=0, tiled=True).reshape(2, shard, -1)
    d_qkv_b = mm(low_one, grad_b, ((0,), (0,))).astype(BF)
    partial = mm(grad_a, w_qkv_a, ((1,), (1,))) + mm(grad_b, w_qkv_b, ((1,), (1,)))
    grad_one = partial[:rows] + swap(partial[rows:].astype(BF))
    result_rows, grad_one = lax.optimization_barrier((result_rows, grad_one))
    layer_output = unsort(result_rows)
    back, gain_one_grad = norm_back(grad_one, gain_one, norm_one, scale_one)
    x = (grad_middle + back).astype(BF).reshape(2, block, width)
    x = jnp.einsum("tri,trd->tid", place_low, x, preferred_element_type=F32).astype(BF)
    x, wide = lax.optimization_barrier((x, wide))
    (x,) = exchange([x.reshape(2, 2, q_count, each, width)], True)
    def finish(terms, after):
        summed, after = reduce_rows(terms, after)
        out = []
        for j, d in enumerate(summed):
            if q_count > 8:
                d = lax.all_gather(d, "sp", axis=0)
            else:
                d = spread(d, (1, 2) if j % 2 == 0 else (2, 1))
            d = d.reshape(2, shard, -1)
            own = lax.dynamic_index_in_dim(d, c, 0, keepdims=False)
            far = swap(lax.dynamic_index_in_dim(d, 1 - c, 0, keepdims=False))
            out.append((own, far))
        return out, after

    def joined(own, far):
        return jnp.where(c == 0, own, far), jnp.where(c == 0, far, own)

    own = lax.dynamic_index_in_dim(wide, c, 0, keepdims=False)
    far = swap(lax.dynamic_index_in_dim(wide, 1 - c, 0, keepdims=False))
    step = wide.shape[2] // 3
    low, high = joined(own, far)
    r_mlp, r_gate, r_up = (
        [x[:, j * step : j * step + half_ff] for x in (low, high)] for j in range(3)
    )
    gain_terms = jnp.pad(jnp.stack([gain_one_grad, gain_two_grad], 1), ((0, 0), (0, 126)))
    (r_out, r_qkv_a, r_qkv_b, r_gain), x = finish(
        [d_out, d_qkv_a, d_qkv_b, gain_terms.astype(BF)], x
    )
    input_grad = unsort(x)
    mlp_grad = jnp.concatenate(r_mlp, 1).T.astype(F32)
    input_grad_w = jnp.concatenate(r_gate + r_up, 1).astype(F32)
    out_grad = jnp.concatenate(joined(*r_out), 1).astype(F32)
    qa, qb = joined(*r_qkv_a), joined(*r_qkv_b)
    third, half = qa[0].shape[1] // 3 * 2, qa[0].shape[1] // 3
    qkv_grad = jnp.concatenate(
        [qa[0][:, :third], qa[1][:, :third]]
        + [qa[0][:, third:], qb[0][:, :half], qa[1][:, third:], qb[1][:, :half]]
        + [qb[0][:, half:], qb[1][:, half:]],
        1,
    ).astype(F32)
    gain_grads = (r_gain[0].astype(F32) + r_gain[1].astype(F32)).T
    return (
        layer_output,
        input_grad,
        qkv_grad,
        out_grad,
        input_grad_w,
        mlp_grad,
        gain_grads[0],
        gain_grads[1],
    )


def solution(mesh):
    sp_count, fsdp_count = mesh.devices.shape
    split = Mesh(mesh.devices.reshape(sp_count, fsdp_count // 2, 2), ("sp", "q", "core"))
    fsdp = ("q", "core")
    big = P(None, fsdp, "sp", None)
    return jax.shard_map(
        on_device,
        mesh=split,
        in_specs=(
            big,
            big,
            P(None, fsdp, "sp"),
            P(None, fsdp, None),
            P(fsdp, None),
            P(fsdp, None),
            P(fsdp, None),
            P(None, fsdp),
            P(fsdp),
            P(fsdp),
        ),
        out_specs=(
            big,
            big,
            P(fsdp, None),
            P(fsdp, None),
            P(fsdp, None),
            P(None, fsdp),
            P(fsdp),
            P(fsdp),
        ),
        check_vma=False,
    )
```
